32 devices in a mesh: row: 8 (over z, core), col: 4 (over y, x).
Axes of the slice: x: 2, y: 2, z: 4, core: 2. Of those that a mesh axis runs over, the one named last changes fastest.
Arguments:
- patches: bfloat16 [3, 128, 128, 1024], P(None, 'row', 'col'), may hold values from -6 to 6
- registers: bfloat16 [3, 8, 1024], replicated, may hold values from -20 to 20
Outputs:
- patch_out: bfloat16 [128, 128, 1024], P('row', 'col')
- register_out: bfloat16 [8, 1024], replicated
The draws below stay inside these ranges and needn't reach their ends.
All inputs are finite; a program needn't handle non-finite values.
Results may differ from the reference program's by a relative error of at most 0.004.
Values may be sent and summed in bfloat16 or wider, within the bound.
No kernel may reach another device: no remote copies, remote signals or barrier semaphores. Data moves between devices by JAX's collectives and lax.ppermute only.
A program may use at most 64 MiB of HBM per device.

```python
import jax
import jax.numpy as jnp
from jax import lax

D = 1024
HEADS = 16
HDIM = 64
RADIUS = 8
REG = 8
HB = 16
WB = 32
NR = 128
NC = 128


def draw_patches(key, part):
    first_key = jax.random.fold_in(jax.random.fold_in(key, 1), 0)
    values_all = jnp.clip(jax.random.normal(first_key, (3, NR, NC, D), jnp.float32), -6.0, 6.0)
    return values_all.astype(jnp.bfloat16)


def draw_registers(key, part):
    first_key = jax.random.fold_in(key, 2)
    spread = jnp.array([3.0, 2.0, 1.0], jnp.float32)[:, None, None]
    values_all = jnp.clip(jax.random.normal(first_key, (3, REG, D), jnp.float32) * spread, -20.0, 20.0)
    return values_all.astype(jnp.bfloat16)


def setup_inputs(seed: int = 0) -> dict:
    arg_keys = jax.random.split(jax.random.key(seed), 3)
    return {
        "patches": draw_patches(jax.random.fold_in(arg_keys[2], 71), 0),
        "registers": draw_registers(jax.random.fold_in(arg_keys[2], 71), 0),
    }


def rounded_f32(values):
    return lax.optimization_barrier(values.astype(jnp.bfloat16)).astype(jnp.float32)


def reference(patches, registers):
    head_size = HDIM
    score_scale = head_size ** -0.5
    padded = jnp.pad(patches[1:3], ((0, 0), (RADIUS, RADIUS), (RADIUS, RADIUS), (0, 0)))
    tiles_down = NR // HB
    tiles_across = NC // WB
    span_rows = HB + 2 * RADIUS
    span_cols = WB + 2 * RADIUS
    query_ids = jnp.arange(HB * WB, dtype=jnp.int32)
    key_ids = jnp.arange(span_rows * span_cols, dtype=jnp.int32)
    query_row = query_ids // WB
    query_col = query_ids % WB
    key_row = key_ids // span_cols
    key_col = key_ids % span_cols
    reg_keys = registers[1].astype(jnp.float32).reshape(REG, HEADS, head_size)
    reg_values = registers[2].astype(jnp.float32).reshape(REG, HEADS, head_size)

    def one_tile(tile_index):
        tile_row = (tile_index // tiles_across).astype(jnp.int32)
        tile_col = (tile_index % tiles_across).astype(jnp.int32)
        zero = jnp.zeros((), jnp.int32)
        queries = lax.dynamic_slice(patches[0], (tile_row * HB, tile_col * WB, zero), (HB, WB, D))
        block = lax.dynamic_slice(padded, (zero, tile_row * HB, tile_col * WB, zero), (2, span_rows, span_cols, D))
        queries = queries.astype(jnp.float32).reshape(HB * WB, HEADS, head_size)
        keys = block[0].astype(jnp.float32).reshape(span_rows * span_cols, HEADS, head_size)
        values = block[1].astype(jnp.float32).reshape(span_rows * span_cols, HEADS, head_size)
        row_gap = key_row[None, :] - RADIUS - query_row[:, None]
        col_gap = key_col[None, :] - RADIUS - query_col[:, None]
        global_row = tile_row * HB + key_row - RADIUS
        global_col = tile_col * WB + key_col - RADIUS
        inside = (jnp.abs(row_gap) <= RADIUS) & (jnp.abs(col_gap) <= RADIUS)
        inside = inside & ((global_row >= 0) & (global_row < NR) & (global_col >= 0) & (global_col < NC))[None, :]
        scores = jnp.einsum("qhd,khd->hqk", queries, keys) * score_scale
        scores = jnp.where(inside[None], scores, -jnp.inf)
        reg_scores = jnp.einsum("qhd,rhd->hqr", queries, reg_keys) * score_scale
        highest = jnp.maximum(jnp.max(scores, axis=2), jnp.max(reg_scores, axis=2))
        weights = jnp.exp(scores - highest[..., None])
        reg_weights = jnp.exp(reg_scores - highest[..., None])
        totals = jnp.sum(weights, axis=2) + jnp.sum(reg_weights, axis=2)
        numerator = jnp.einsum("hqk,khd->qhd", rounded_f32(weights), values)
        numerator = numerator + jnp.einsum("hqr,rhd->qhd", rounded_f32(reg_weights), reg_values)
        result = numerator / jnp.transpose(totals)[..., None]
        return result.reshape(HB, WB, D).astype(jnp.bfloat16)

    tiles = lax.map(one_tile, jnp.arange(tiles_down * tiles_across, dtype=jnp.int32))
    tiles = tiles.reshape(tiles_down, tiles_across, HB, WB, D)
    patch_out = jnp.transpose(tiles, (0, 2, 1, 3, 4)).reshape(NR, NC, D)

    reg_queries = registers[0].astype(jnp.float32).reshape(REG, HEADS, head_size)
    all_keys = patches[1].astype(jnp.float32).reshape(NR * NC, HEADS, head_size)
    all_values = patches[2].astype(jnp.float32).reshape(NR * NC, HEADS, head_size)
    scores = jnp.einsum("rhd,khd->hrk", reg_queries, all_keys) * score_scale
    self_scores = jnp.einsum("rhd,shd->hrs", reg_queries, reg_keys) * score_scale
    highest = jnp.maximum(jnp.max(scores, axis=2), jnp.max(self_scores, axis=2))
    weights = jnp.exp(scores - highest[..., None])
    self_weights = jnp.exp(self_scores - highest[..., None])
    totals = jnp.sum(weights, axis=2) + jnp.sum(self_weights, axis=2)
    numerator = jnp.einsum("hrk,khd->hrd", rounded_f32(weights), all_values)
    numerator = numerator + jnp.einsum("hrs,shd->hrd", rounded_f32(self_weights), reg_values)
    register_out = jnp.transpose(numerator / totals[..., None], (1, 0, 2)).reshape(REG, D).astype(jnp.bfloat16)
    return patch_out, register_out
```

```python
import functools

import jax
import jax.numpy as jnp
from jax import lax
from jax.experimental import pallas as pl
from jax.experimental.pallas import tpu as pltpu
from jax.sharding import PartitionSpec as P

HEADS = 16
RADIUS = 8
FAR = -30000.0
F32 = jnp.float32
BF16 = jnp.bfloat16
NT = (((1,), (1,)), ((), ()))
NN = (((1,), (0,)), ((), ()))
TN = (((0,), (0,)), ((), ()))


def dot(a, b, dims):
    return lax.dot_general(a, b, dims, preferred_element_type=F32)


def shift(x, axis, step):
    n = lax.axis_size(axis)
    return lax.ppermute(x, axis, [(i, i + step) for i in range(n) if 0 <= i + step < n])


def key_features(rows, cols, grid_ok, tile_rows, tile_cols):
    lane = jnp.arange(128, dtype=jnp.int32)[None, :]
    far_col = (lane < tile_cols) & (jnp.abs(cols[:, None] - lane) > RADIUS)
    row_lane = lane - tile_cols
    is_row = (row_lane >= 0) & (row_lane < tile_rows)
    far_row = is_row & (jnp.abs(rows[:, None] - row_lane) > RADIUS)
    off = (lane == tile_cols + tile_rows) & ~grid_ok[:, None]
    return jnp.where(far_col | far_row | off, FAR, 0.0).astype(BF16)


def query_features(rows, cols, tile_rows, tile_cols):
    lane = jnp.arange(128, dtype=jnp.int32)[None, :]
    hit = (lane == cols[:, None]) | (lane == tile_cols + rows[:, None])
    return (hit | (lane == tile_cols + tile_rows)).astype(BF16)


def register_kernel(scale, flag_ref, reg_ref, k_ref, v_ref, out_ref):
    count = reg_ref.shape[1]
    width = reg_ref.shape[2]
    head = width // HEADS
    keys = k_ref[...].reshape(-1, width)
    values = v_ref[...].reshape(-1, width)
    lane_head = lax.broadcasted_iota(jnp.int32, (HEADS, count, width), 2) // head
    own = lane_head == lax.broadcasted_iota(jnp.int32, (HEADS, count, width), 0)
    q = reg_ref[0].astype(F32) * scale
    q = jnp.where(own, q[None], 0.0).reshape(HEADS * count, width).astype(BF16)
    scores = dot(keys, q, NT)
    self_scores = dot(reg_ref[1], q, NT) + flag_ref[0]
    high = jnp.maximum(
        jnp.max(scores, axis=0, keepdims=True), jnp.max(self_scores, axis=0, keepdims=True)
    )
    w = jnp.exp(scores - high)
    self_w = jnp.exp(self_scores - high)
    total = jnp.sum(w, axis=0, keepdims=True) + jnp.sum(self_w, axis=0, keepdims=True)
    acc = dot(jnp.transpose(w).astype(BF16), values, NN)
    acc = acc + dot(jnp.transpose(self_w).astype(BF16), reg_ref[2], NN)
    acc = jnp.sum(jnp.where(own, acc.reshape(HEADS, count, width), 0.0), axis=0)
    n = HEADS * count

    def spread(row):
        col = jnp.transpose(jnp.broadcast_to(row, (128, n))).reshape(HEADS, count, 128)
        low = lax.broadcasted_iota(jnp.int32, (count, 128), 1) < head
        return jnp.concatenate(
            [jnp.where(low, col[2 * p], col[2 * p + 1]) for p in range(HEADS // 2)], axis=1
        )

    out_ref[0] = acc
    out_ref[1] = spread(high)
    out_ref[2] = spread(total)


def register_partial(patches, registers, flag, scale):
    _, tr, tc, width = patches.shape
    count = registers.shape[1]
    return pl.pallas_call(
        functools.partial(register_kernel, scale),
        grid=(1,),
        in_specs=[
            pl.BlockSpec(memory_space=pltpu.SMEM),
            pl.BlockSpec((3, count, width), lambda i: (0, 0, 0)),
            pl.BlockSpec((None, tr, tc, width), lambda i: (1, 0, 0, 0)),
            pl.BlockSpec((None, tr, tc, width), lambda i: (2, 0, 0, 0)),
        ],
        out_specs=pl.BlockSpec((3, count, width), lambda i: (0, 0, 0)),
        out_shape=jax.ShapeDtypeStruct((3, count, width), F32),
        cost_estimate=pl.CostEstimate(flops=300_000_000, bytes_accessed=2_200_000, transcendentals=70_000),
        name="register_part",
    )(flag, registers, patches, patches)


def merge(a, b):
    high = jnp.maximum(a[1], b[1])
    fa = jnp.exp(a[1] - high)
    fb = jnp.exp(b[1] - high)
    return jnp.stack([a[0] * fa + b[0] * fb, high, a[2] * fa + b[2] * fb])


def merge_over(part, axis):
    n = lax.axis_size(axis)
    if n & (n - 1):
        every = lax.all_gather(part, axis)
        return functools.reduce(merge, [every[i] for i in range(n)])
    step = 1
    while step < n:
        part = merge(part, lax.ppermute(part, axis, [(i, i ^ step) for i in range(n)]))
        step *= 2
    return part


def by_column_group(x, groups):
    r, c, d = x.shape
    g = c // groups
    return jnp.concatenate(
        [x[:, i * g : (i + 1) * g].reshape(r * g, d) for i in range(groups)], axis=0
    )


def centre_kernel(scale, q_ref, k_ref, v_ref, up_ref, down_ref, reg_ref, qf_ref, kf_ref, out_ref, st_ref):
    tr, tc, d = q_ref.shape
    half_rows = tr // 2
    head = d // 2
    nq = half_rows * tc
    edge = half_rows * RADIUS
    groups = tc // RADIUS
    low_q = lax.broadcasted_iota(jnp.int32, (nq, d), 1) < head
    k_own = k_ref[...].reshape(tr * tc, d)
    v_own = v_ref[...].reshape(tr * tc, d)
    reg_k = jnp.concatenate([reg_ref[1], jnp.zeros_like(reg_ref[1])], axis=0)
    reg_v = jnp.concatenate([reg_ref[2], jnp.zeros_like(reg_ref[2])], axis=0)
    nr = reg_k.shape[0]
    last = lax.broadcasted_iota(jnp.int32, (nr, 128), 1) == tr + tc
    pad_row = lax.broadcasted_iota(jnp.int32, (nr, 128), 0) >= nr // 2
    reg_f = jnp.where(last & pad_row, FAR, 0.0).astype(BF16)
    for half in range(2):
        if half == 0:
            k = [up_ref[0].reshape(-1, d), k_own]
            v = [up_ref[1].reshape(-1, d), v_own]
            f0 = 0
        else:
            k = [k_own, down_ref[0].reshape(-1, d)]
            v = [v_own, down_ref[1].reshape(-1, d)]
            f0 = RADIUS * tc
        k = jnp.concatenate(k + [reg_k], axis=0)
        v = jnp.concatenate(v + [reg_v], axis=0)
        f = jnp.concatenate([kf_ref[f0 : f0 + (tr + RADIUS) * tc], reg_f], axis=0)
        kc = jnp.concatenate([k, f], axis=1)
        q = q_ref[half * half_rows : (half + 1) * half_rows].astype(F32) * scale
        q = by_column_group(q, groups)
        qf = qf_ref[half * nq : (half + 1) * nq]
        low_v = lax.broadcasted_iota(jnp.int32, v.shape, 1) < head
        one = jnp.ones_like(v)
        outs, highs = [], []
        for side in range(2):
            mine = low_q if side == 0 else ~low_q
            qc = jnp.concatenate([jnp.where(mine, q, 0.0).astype(BF16), qf], axis=1)
            s = dot(kc, qc, NT)
            high = jnp.max(s, axis=0, keepdims=True)
            w = jnp.exp(s - high).astype(BF16)
            va = jnp.where(low_v, v, one) if side == 0 else jnp.where(low_v, one, v)
            outs.append(dot(va, w, TN))
            highs.append(high)
        oa, ob = outs
        o = jnp.concatenate([oa[:head] / oa[head:], ob[head:] / ob[:head]], axis=0)
        o = jnp.transpose(o).reshape(groups, half_rows, RADIUS, d)
        o = jnp.concatenate([o[g] for g in range(groups)], axis=1)
        out_ref[half * half_rows : (half + 1) * half_rows] = o.astype(BF16)
        for side in range(2):
            c0 = 0 if side == 0 else nq - edge
            cut = lambda a, b: jnp.concatenate([a[:, c0 : c0 + edge], b[:, c0 : c0 + edge]], axis=1)
            st_ref[half, side, :d] = cut(oa, ob)
            high = cut(highs[0], highs[1])
            total = cut(oa[head : head + 1], ob[0:1])
            st_ref[half, side, d : d + 8] = jnp.concatenate(
                [high, total, jnp.zeros((6, 2 * edge), F32)], axis=0
            )


def centre(patches, up, down, registers, qf, kf, scale):
    _, tr, tc, width = patches.shape
    pairs = HEADS // 2
    d = width // pairs
    count = registers.shape[1]
    edge = tr // 2 * RADIUS
    part = lambda j: pl.BlockSpec((None, tr, tc, d), lambda p, j=j: (j, 0, 0, p))
    keys = (tr + RADIUS) * tc + 2 * count
    halo = pl.BlockSpec((2, RADIUS, tc, d), lambda p: (0, 0, 0, p))
    return pl.pallas_call(
        functools.partial(centre_kernel, scale),
        grid=(pairs,),
        in_specs=[
            part(0),
            part(1),
            part(2),
            halo,
            halo,
            pl.BlockSpec((3, count, d), lambda p: (0, 0, p)),
            pl.BlockSpec(qf.shape, lambda p: (0, 0)),
            pl.BlockSpec(kf.shape, lambda p: (0, 0)),
        ],
        out_specs=[
            pl.BlockSpec((tr, tc, d), lambda p: (0, 0, p)),
            pl.BlockSpec((None, 2, 2, d + 8, 2 * edge), lambda p: (p, 0, 0, 0, 0)),
        ],
        out_shape=[
            jax.ShapeDtypeStruct((tr, tc, width), BF16),
            jax.ShapeDtypeStruct((pairs, 2, 2, d + 8, 2 * edge), F32),
        ],
        cost_estimate=pl.CostEstimate(
            flops=HEADS * keys * tr * tc * 2 * 384,
            bytes_accessed=8_000_000,
            transcendentals=HEADS * keys * tr * tc,
        ),
        name="centre",
    )(patches, patches, patches, up, down, registers, qf, kf)


def edge_kernel(scale, q_ref, l_ref, r_ref, cu_ref, cd_ref, qf_ref, kf_ref, st_ref, prev_ref, out_ref):
    tr, tc, d = q_ref.shape
    half_rows = tr // 2
    head = d // 2
    edge = half_rows * RADIUS
    nq = half_rows * tc
    low = lax.broadcasted_iota(jnp.int32, (edge, d), 1) < head
    span = (tr + RADIUS) * RADIUS
    for half in range(2):
        rows = slice(half * half_rows, (half + 1) * half_rows)
        q_rows = q_ref[rows].astype(F32) * scale
        done = []
        for side in range(2):
            halo = l_ref if side == 0 else r_ref
            corner = cu_ref if half == 0 else cd_ref
            c0 = 0 if side == 0 else RADIUS

            def keys(j):
                own = halo[j].astype(F32).reshape(tr * RADIUS, d)
                cor = corner[j].astype(F32)[:, c0 : c0 + RADIUS].reshape(RADIUS * RADIUS, d)
                both = [cor, own] if half == 0 else [own, cor]
                return jnp.concatenate(both, axis=0).astype(BF16)

            f0 = side * (tr + 2 * RADIUS) * RADIUS + half * RADIUS * RADIUS
            kc = jnp.concatenate([keys(0), kf_ref[f0 : f0 + span]], axis=1)
            v = keys(1)
            x0 = 0 if side == 0 else tc - RADIUS
            q = q_rows[:, x0 : x0 + RADIUS].reshape(edge, d)
            q2 = jnp.concatenate([jnp.where(low, q, 0.0), jnp.where(low, 0.0, q)], axis=0)
            g0 = half * nq + (0 if side == 0 else nq - edge)
            qf = qf_ref[g0 : g0 + edge]
            qc = jnp.concatenate([q2.astype(BF16), jnp.concatenate([qf, qf], axis=0)], axis=1)
            s = dot(kc, qc, NT)
            high1 = st_ref[half, side, d : d + 1]
            total1 = st_ref[half, side, d + 1 : d + 2]
            high = jnp.maximum(high1, jnp.max(s, axis=0, keepdims=True))
            fade = jnp.exp(high1 - high)
            w = jnp.exp(s - high)
            total = total1 * fade + jnp.sum(w, axis=0, keepdims=True)
            acc = st_ref[half, side, :d] * fade + dot(v, w.astype(BF16), TN)
            o = jnp.transpose(acc / total)
            o = jnp.where(low, o[:edge], o[edge:])
            done.append(o.reshape(half_rows, RADIUS, d))
        mid = prev_ref[rows].astype(F32)[:, RADIUS : tc - RADIUS]
        out_ref[rows] = jnp.concatenate([done[0], mid, done[1]], axis=1).astype(BF16)


def edges(patches, left, right, corner_up, corner_down, qf, kf, state, prev, scale):
    _, tr, tc, width = patches.shape
    pairs = HEADS // 2
    d = width // pairs
    side = pl.BlockSpec((2, tr, RADIUS, d), lambda p: (0, 0, 0, p))
    corner = pl.BlockSpec((2, RADIUS, 2 * RADIUS, d), lambda p: (0, 0, 0, p))
    tile = pl.BlockSpec((tr, tc, d), lambda p: (0, 0, p))
    return pl.pallas_call(
        functools.partial(edge_kernel, scale),
        grid=(pairs,),
        in_specs=[
            pl.BlockSpec((None, tr, tc, d), lambda p: (0, 0, 0, p)),
            side,
            side,
            corner,
            corner,
            pl.BlockSpec(qf.shape, lambda p: (0, 0)),
            pl.BlockSpec(kf.shape, lambda p: (0, 0)),
            pl.BlockSpec((None,) + state.shape[1:], lambda p: (p, 0, 0, 0, 0)),
            tile,
        ],
        out_specs=tile,
        out_shape=jax.ShapeDtypeStruct((tr, tc, width), BF16),
        input_output_aliases={8: 0},
        cost_estimate=pl.CostEstimate(flops=500_000_000, bytes_accessed=6_000_000, transcendentals=800_000),
        name="edges",
    )(patches, left, right, corner_up, corner_down, qf, kf, state, prev)


def local(patches, registers):
    _, tr, tc, width = patches.shape
    scale = (width // HEADS) ** (-0.5)
    row_at, row_n = lax.axis_index("row"), lax.axis_size("row")
    col_at, col_n = lax.axis_index("col"), lax.axis_size("col")
    kv = patches[1:3]

    left = shift(kv[:, :, tc - RADIUS :], "col", 1)
    right = shift(kv[:, :, :RADIUS], "col", -1)
    up = shift(kv[:, tr - RADIUS :], "row", 1)
    down = shift(kv[:, :RADIUS], "row", -1)

    flag = jnp.where((row_at == 0) & (col_at == 0), 0.0, -1e30).astype(F32).reshape(1)
    part = register_partial(patches, registers, flag, scale)
    part = merge_over(merge_over(part, "row"), "col")
    register_out = (part[0] / part[2]).astype(BF16)

    key_rows = jnp.arange(-RADIUS, tr + RADIUS, dtype=jnp.int32)
    row_ok = ((key_rows >= 0) | (row_at > 0)) & ((key_rows < tr) | (row_at < row_n - 1))

    def features(cols, col_ok):
        n = cols.shape[0]
        rows = jnp.repeat(key_rows, n)
        ok = jnp.repeat(row_ok, n) & col_ok
        return key_features(rows, jnp.tile(cols, tr + 2 * RADIUS), ok, tr, tc)

    arange = lambda a, b: jnp.arange(a, b, dtype=jnp.int32)
    kf = features(arange(0, tc), True)
    kf_side = jnp.concatenate(
        [
            features(arange(-RADIUS, 0), col_at > 0),
            features(arange(tc, tc + RADIUS), col_at < col_n - 1),
        ]
    )
    q_id = arange(0, tr * tc).reshape(2, tc // RADIUS, tr // 2, RADIUS)
    at = lambda i: lax.broadcasted_iota(jnp.int32, q_id.shape, i)
    q_rows = (at(0) * (tr // 2) + at(2)).reshape(-1)
    q_cols = (at(1) * RADIUS + at(3)).reshape(-1)
    qf = query_features(q_rows, q_cols, tr, tc)

    out, state = centre(patches, up, down, registers, qf, kf, scale)
    halo = jnp.concatenate([left, right], axis=2)
    corner_up = shift(halo[:, tr - RADIUS :], "row", 1)
    corner_down = shift(halo[:, :RADIUS], "row", -1)
    out = edges(patches, left, right, corner_up, corner_down, qf, kf_side, state, out, scale)
    return (out, register_out)


def solution(mesh):
    in_specs = (P(None, "row", "col", None), P())
    out_specs = (P("row", "col", None), P())
    return jax.shard_map(local, mesh=mesh, in_specs=in_specs, out_specs=out_specs, check_vma=False)
```

```python
import functools

import jax
import jax.numpy as jnp
import numpy as np
from jax import lax
from jax.experimental import pallas as pl
from jax.experimental.pallas import tpu as pltpu
from jax.sharding import PartitionSpec as P

HEADS = 16
RADIUS = 8
FAR = -30000.0
LANES = 128
F32 = jnp.float32
BF16 = jnp.bfloat16
NT = (((1,), (1,)), ((), ()))
NN = (((1,), (0,)), ((), ()))
TN = (((0,), (0,)), ((), ()))
VMEM = pl.BlockSpec(memory_space=pltpu.VMEM)
HBM = pl.BlockSpec(memory_space=pltpu.HBM)
SMEM = pl.BlockSpec(memory_space=pltpu.SMEM)
PARAMS = pltpu.CompilerParams(vmem_limit_bytes=24 * 1024 * 1024)


def dot(a, b, dims):
    return lax.dot_general(a, b, dims, preferred_element_type=F32)


def shift(x, axis, step):
    n = lax.axis_size(axis)
    return lax.ppermute(x, axis, [(i, i + step) for i in range(n) if 0 <= i + step < n])


def key_features(rows, cols, tr, tc):
    lane = np.arange(LANES)
    far_col = (lane < tc) & (np.abs(cols[..., None] - lane) > RADIUS)
    far_row = (lane >= tc) & (lane < tc + tr) & (np.abs(rows[..., None] - (lane - tc)) > RADIUS)
    return np.where(far_col | far_row, FAR, 0.0).astype(np.float32)


def query_features(rows, cols, tr, tc):
    lane = np.arange(LANES)
    hit = (lane == cols[..., None]) | (lane - tc == rows[..., None]) | (lane == tc + tr)
    return hit.astype(np.float32)


def with_grid_edge(const, off):
    lane = lax.broadcasted_iota(jnp.int32, const.shape, const.ndim - 1)
    return jnp.where((lane == off[1]) & off[0], FAR, jnp.asarray(const)).astype(BF16)


def copy_all(copies, sems):
    started = []
    for i, (src, dst) in enumerate(copies):
        c = pltpu.make_async_copy(src, dst, sems.at[i])
        c.start()
        started.append(c)
    return started


def pack_kernel(p_ref, right_ref, left_ref, down_ref, up_ref, sems):
    _, tr, tc, _ = p_ref.shape
    groups = tc // RADIUS
    copies = []
    for j in range(2):
        copies.append((p_ref.at[1 + j, :, pl.ds(tc - RADIUS, RADIUS)], right_ref.at[j]))
        copies.append((p_ref.at[1 + j, :, pl.ds(0, RADIUS)], left_ref.at[j]))
    for j in range(2):
        for g in range(groups):
            cols = pl.ds(g * RADIUS, RADIUS)
            copies.append((p_ref.at[1 + j, pl.ds(tr - RADIUS, RADIUS), cols], down_ref.at[j, g]))
            copies.append((p_ref.at[1 + j, pl.ds(0, RADIUS), cols], up_ref.at[j, g]))
    for c in copy_all(copies, sems):
        c.wait()


def pack(patches):
    _, tr, tc, width = patches.shape
    groups = tc // RADIUS
    side = pltpu.VMEM((2, tr, RADIUS, width), BF16)
    rows = pltpu.VMEM((2, groups, RADIUS, RADIUS, width), BF16)
    return pl.pallas_call(
        pack_kernel,
        in_specs=[HBM],
        out_specs=[VMEM] * 4,
        out_shape=[side, side, rows, rows],
        scratch_shapes=[pltpu.SemaphoreType.DMA((4 + 4 * groups,))],
        compiler_params=PARAMS,
        name="pack",
    )(patches)


def prep_kernel(scale, flag_ref, reg_ref, p_ref, out_ref, part_ref, sems):
    _, tr, tc, width = p_ref.shape
    groups = tc // RADIUS
    count = reg_ref.shape[1]
    head = width // HEADS
    copies = [
        (p_ref.at[j, :, pl.ds(g * RADIUS, RADIUS)], out_ref.at[j, g])
        for j in (1, 2, 0)
        for g in range(groups)
    ]
    started = copy_all(copies, sems)
    lane_head = lax.broadcasted_iota(jnp.int32, (HEADS, count, width), 2) // head
    own = lane_head == lax.broadcasted_iota(jnp.int32, (HEADS, count, width), 0)
    q = reg_ref[0].astype(F32) * scale
    q = jnp.where(own, q[None], 0.0).reshape(HEADS * count, width).astype(BF16)
    self_scores = dot(reg_ref[1], q, NT) + flag_ref[0]
    for c in started[:groups]:
        c.wait()
    scores = dot(out_ref[1].reshape(tr * tc, width), q, NT)
    high = jnp.maximum(
        jnp.max(scores, axis=0, keepdims=True), jnp.max(self_scores, axis=0, keepdims=True)
    )
    w = jnp.exp(scores - high)
    self_w = jnp.exp(self_scores - high)
    total = jnp.sum(w, axis=0, keepdims=True) + jnp.sum(self_w, axis=0, keepdims=True)
    wt = jnp.transpose(w).astype(BF16)
    for c in started[groups:]:
        c.wait()
    acc = dot(wt, out_ref[2].reshape(tr * tc, width), NN)
    acc = acc + dot(jnp.transpose(self_w).astype(BF16), reg_ref[2], NN)
    acc = jnp.sum(jnp.where(own, acc.reshape(HEADS, count, width), 0.0), axis=0)
    n = HEADS * count

    def spread(row):
        col = jnp.transpose(jnp.broadcast_to(row, (LANES, n))).reshape(HEADS, count, LANES)
        low = lax.broadcasted_iota(jnp.int32, (count, LANES), 1) < head
        return jnp.concatenate(
            [jnp.where(low, col[2 * p], col[2 * p + 1]) for p in range(HEADS // 2)], axis=1
        )

    part_ref[0] = acc
    part_ref[1] = spread(high)
    part_ref[2] = spread(total)


def prep(patches, registers, flag, scale):
    _, tr, tc, width = patches.shape
    groups = tc // RADIUS
    count = registers.shape[1]
    return pl.pallas_call(
        functools.partial(prep_kernel, scale),
        in_specs=[SMEM, VMEM, HBM],
        out_specs=[VMEM, VMEM],
        out_shape=[
            pltpu.VMEM((3, groups, tr, RADIUS, width), BF16),
            pltpu.VMEM((3, count, width), F32),
        ],
        scratch_shapes=[pltpu.SemaphoreType.DMA((3 * groups,))],
        cost_estimate=pl.CostEstimate(
            flops=300_000_000, bytes_accessed=4_000_000, transcendentals=70_000
        ),
        compiler_params=PARAMS,
        name="prep",
    )(flag, registers, patches)


def merge(a, b):
    high = jnp.maximum(a[1], b[1])
    fa = jnp.exp(a[1] - high)
    fb = jnp.exp(b[1] - high)
    return jnp.stack([a[0] * fa + b[0] * fb, high, a[2] * fa + b[2] * fb])


def merge_over(part, axis):
    n = lax.axis_size(axis)
    if n & (n - 1):
        every = lax.all_gather(part, axis)
        return functools.reduce(merge, [every[i] for i in range(n)])
    step = 1
    while step < n:
        part = merge(part, lax.ppermute(part, axis, [(i, i ^ step) for i in range(n)]))
        step *= 2
    return part


def centre_kernel(scale, first, p_ref, up_ref, down_ref, reg_ref, qf_ref, kf_ref, in_ref, st_ref):
    _, groups, cells, width = p_ref.shape
    d = LANES
    head = width // HEADS
    edge = RADIUS * RADIUS
    low = lax.broadcasted_iota(jnp.int32, (edge, d), 1) < head
    pad = lax.broadcasted_iota(jnp.int32, (2 * RADIUS, d), 0) >= RADIUS
    off = lax.broadcasted_iota(jnp.int32, (2 * RADIUS, d), 1) == d - 1
    reg_f = jnp.where(pad & off, FAR, 0.0).astype(BF16)
    zero = jnp.zeros((RADIUS, d), BF16)

    @pl.loop(0, st_ref.shape[0])
    def _(i):
        lanes = pl.ds(pl.multiple_of((i + first) * d, d), d)
        lanes_out = pl.ds(pl.multiple_of(i * d, d), d)
        reg_k = jnp.concatenate([reg_ref[1, :, lanes], zero], axis=0)
        reg_v = jnp.concatenate([reg_ref[2, :, lanes], zero], axis=0)
        for half in range(2):
            for part in range(2):
                near = range(part, part + 3)

                def piece(j, g):
                    own = p_ref[1 + j, g, :, lanes]
                    if half == 0:
                        return [up_ref[j, g, :, lanes], own]
                    return [own, down_ref[j, g, :, lanes]]

                span = cells + edge
                k = jnp.concatenate(sum([piece(0, g) for g in near], []) + [reg_k], axis=0)
                v = jnp.concatenate(sum([piece(1, g) for g in near], []) + [reg_v], axis=0)
                f = jnp.concatenate(
                    [kf_ref[g, half * edge : half * edge + span] for g in near] + [reg_f], axis=0
                )
                kc = jnp.concatenate([k, f], axis=1)
                qs = []
                for g in (0, 1) if part == 0 else (3, 2):
                    rows = slice(half * edge, (half + 1) * edge)
                    q = p_ref[0, g, rows, lanes].astype(F32) * scale
                    qf = qf_ref[g, rows]
                    for x in (jnp.where(low, q, 0.0), jnp.where(low, 0.0, q)):
                        qs.append(jnp.concatenate([x.astype(BF16), qf], axis=1))
                s = dot(kc, jnp.concatenate(qs, axis=0), NT)
                high = jnp.max(s, axis=0, keepdims=True)
                w = jnp.exp(s - high)
                total = jnp.sum(w, axis=0, keepdims=True)
                o = dot(v, w.astype(BF16), TN)
                st_ref[i, half, part, :d] = o[:, :d]
                st_ref[i, half, part, d : d + 8] = jnp.concatenate(
                    [high[:, :d], total[:, :d], jnp.zeros((6, d), F32)], axis=0
                )
                t = jnp.transpose(o[:, d:] / total[:, d:])
                t = jnp.where(low, t[:edge], t[edge:])
                in_ref[part, half * edge : (half + 1) * edge, lanes_out] = t.astype(BF16)


def centre(pg, up, down, registers, qf, kf, scale, first, pairs):
    _, groups, cells, width = pg.shape
    edge = RADIUS * RADIUS
    d = LANES
    keys = 3 * (cells + edge) + 2 * RADIUS
    work = pairs * 4 * keys * 4 * edge
    return pl.pallas_call(
        functools.partial(centre_kernel, scale, first),
        in_specs=[VMEM] * 6,
        out_specs=[VMEM, VMEM],
        out_shape=[
            pltpu.VMEM((2, cells, pairs * d), BF16),
            pltpu.VMEM((pairs, 2, 2, d + 8, d), F32),
        ],
        cost_estimate=pl.CostEstimate(
            flops=work * 2 * 384, bytes_accessed=4_000_000, transcendentals=work
        ),
        compiler_params=PARAMS,
        name="centre",
    )(pg, up, down, registers, qf, kf)


def edge_kernel(
    scale, parts, p_ref, l_ref, r_ref, cu_ref, cd_ref, qf_ref, kf_ref, *refs
):
    inner, states = refs[:parts], refs[parts : 2 * parts]
    out_ref, edge_ref, sems = refs[2 * parts :]
    _, groups, cells, width = p_ref.shape
    d = LANES
    head = width // HEADS
    edge = RADIUS * RADIUS
    span = cells + edge
    low = lax.broadcasted_iota(jnp.int32, (edge, d), 1) < head
    per = states[0].shape[0]
    copies = []
    for n in range(parts):
        for part in range(2):
            g = 1 if part == 0 else groups - 2
            copies.append(
                (
                    inner[n].at[part],
                    out_ref.at[:, pl.ds(g * RADIUS, RADIUS), pl.ds(n * per * d, per * d)],
                )
            )
    started = copy_all(copies, sems)
    for n in range(parts):

        @pl.loop(0, per)
        def _(i):
            lanes = pl.ds(pl.multiple_of((i + n * per) * d, d), d)
            for half in range(2):
                cells_of = slice(half * edge, (half + 1) * edge)
                for side in range(2):
                    halo = l_ref if side == 0 else r_ref
                    corner = cu_ref if half == 0 else cd_ref

                    def keys(j):
                        own = halo[j, :, lanes]
                        far = corner[j, side, :, lanes]
                        return jnp.concatenate([far, own] if half == 0 else [own, far], axis=0)

                    f = kf_ref[side, half * edge : half * edge + span]
                    kc = jnp.concatenate([keys(0), f], axis=1)
                    g = 0 if side == 0 else groups - 1
                    q = p_ref[0, g, cells_of, lanes].astype(F32) * scale
                    qf = qf_ref[g, cells_of]
                    qc = jnp.concatenate(
                        [
                            jnp.concatenate([x.astype(BF16), qf], axis=1)
                            for x in (jnp.where(low, q, 0.0), jnp.where(low, 0.0, q))
                        ],
                        axis=0,
                    )
                    s = dot(kc, qc, NT)
                    st = states[n]
                    high1 = st[i, half, side, d : d + 1]
                    total1 = st[i, half, side, d + 1 : d + 2]
                    high = jnp.maximum(high1, jnp.max(s, axis=0, keepdims=True))
                    fade = jnp.exp(high1 - high)
                    w = jnp.exp(s - high)
                    total = total1 * fade + jnp.sum(w, axis=0, keepdims=True)
                    acc = st[i, half, side, :d] * fade + dot(keys(1), w.astype(BF16), TN)
                    t = jnp.transpose(acc / total)
                    t = jnp.where(low, t[:edge], t[edge:])
                    rows_of = slice(half * RADIUS, (half + 1) * RADIUS)
                    edge_ref[side, rows_of, :, lanes] = t.reshape(RADIUS, RADIUS, d).astype(BF16)

    copies = []
    for side in range(2):
        g = 0 if side == 0 else groups - 1
        copies.append(
            (edge_ref.at[side], out_ref.at[:, pl.ds(g * RADIUS, RADIUS)])
        )
    started += copy_all(copies, sems.at[pl.ds(2 * parts, 2)])
    for c in started:
        c.wait()


def edges(pg, left, right, corner_up, corner_down, qf, kf, inner, states, scale, tr, tc):
    _, groups, cells, width = pg.shape
    parts = len(states)
    return pl.pallas_call(
        functools.partial(edge_kernel, scale, parts),
        in_specs=[VMEM] * (7 + 2 * parts),
        out_specs=HBM,
        out_shape=jax.ShapeDtypeStruct((tr, tc, width), BF16),
        scratch_shapes=[
            pltpu.VMEM((2, tr, RADIUS, width), BF16),
            pltpu.SemaphoreType.DMA((2 * parts + 2,)),
        ],
        cost_estimate=pl.CostEstimate(
            flops=500_000_000, bytes_accessed=3_000_000, transcendentals=800_000
        ),
        compiler_params=PARAMS,
        name="edges",
    )(pg, left, right, corner_up, corner_down, qf, kf, *inner, *states)


def local(patches, registers):
    _, tr, tc, width = patches.shape
    groups = tc // RADIUS
    cells = tr * RADIUS
    edge = RADIUS * RADIUS
    assert tr == 2 * RADIUS and groups == 4 and 2 * width == HEADS * LANES
    scale = (width // HEADS) ** (-0.5)
    row_at, row_n = lax.axis_index("row"), lax.axis_size("row")
    col_at, col_n = lax.axis_index("col"), lax.axis_size("col")

    to_right, to_left, to_down, to_up = pack(patches)
    left = shift(to_right, "col", 1).reshape(2, cells, width)
    right = shift(to_left, "col", -1).reshape(2, cells, width)
    up = shift(to_down, "row", 1).reshape(2, groups, edge, width)
    down = shift(to_up, "row", -1).reshape(2, groups, edge, width)

    flag = jnp.where((row_at == 0) & (col_at == 0), 0.0, -1e30).astype(F32).reshape(1)
    pg, part = prep(patches, registers, flag, scale)
    pg = pg.reshape(3, groups, cells, width)
    part = merge_over(merge_over(part, "row"), "col")
    register_out = (part[0] / part[2]).astype(BF16)

    key_rows = np.repeat(np.arange(-RADIUS, tr + RADIUS), RADIUS)
    key_cols = np.tile(np.arange(RADIUS), tr + 2 * RADIUS)
    stack = lambda cols: np.stack([key_features(key_rows, key_cols + c, tr, tc) for c in cols])
    row = jnp.arange((tr + 2 * RADIUS) * RADIUS, dtype=jnp.int32)[None, :, None]
    off_rows = ((row < edge) & (row_at == 0)) | ((row >= edge + cells) & (row_at == row_n - 1))
    side = jnp.arange(2, dtype=jnp.int32)[:, None, None]
    off_cols = ((side == 0) & (col_at == 0)) | ((side == 1) & (col_at == col_n - 1))
    off_lane = LANES - 1
    kf = with_grid_edge(stack([g * RADIUS for g in range(groups)]), (off_rows, off_lane))
    kf_side = with_grid_edge(stack([-RADIUS, tc]), (off_rows | off_cols, off_lane))
    q_rows = np.repeat(np.arange(tr), RADIUS)
    q_cols = np.tile(np.arange(RADIUS), tr)
    qf = np.stack([query_features(q_rows, q_cols + g * RADIUS, tr, tc) for g in range(groups)])
    qf[..., off_lane] = 1.0
    qf = jnp.asarray(qf.astype(BF16))

    pairs = HEADS // 2
    parts = 2
    per = pairs // parts
    done = [centre(pg, up, down, registers, qf, kf, scale, n * per, per) for n in range(parts)]
    corner_up = shift(jnp.stack([left[:, -edge:], right[:, -edge:]], axis=1), "row", 1)
    corner_down = shift(jnp.stack([left[:, :edge], right[:, :edge]], axis=1), "row", -1)
    inner = [x[0].reshape(2, tr, RADIUS, per * LANES) for x in done]
    out = edges(
        pg, left, right, corner_up, corner_down, qf, kf_side, inner, [x[1] for x in done], scale, tr, tc
    )
    return (out, register_out)


def solution(mesh):
    in_specs = (P(None, "row", "col", None), P())
    out_specs = (P("row", "col", None), P())
    return jax.shard_map(local, mesh=mesh, in_specs=in_specs, out_specs=out_specs, check_vma=False)
```

```python
import functools

import jax
import jax.numpy as jnp
import numpy as np
from jax import lax
from jax.experimental import pallas as pl
from jax.experimental.pallas import tpu as pltpu
from jax.sharding import PartitionSpec as P


HEADS = 16
PARTS = 4
RADIUS = 8
FAR = -30000.0
LANES = 128
F32 = jnp.float32
BF16 = jnp.bfloat16
NT = (((1,), (1,)), ((), ()))
NN = (((1,), (0,)), ((), ()))
TN = (((0,), (0,)), ((), ()))
VMEM = pl.BlockSpec(memory_space=pltpu.VMEM)
HBM = pl.BlockSpec(memory_space=pltpu.HBM)
SMEM = pl.BlockSpec(memory_space=pltpu.SMEM)
PARAMS = pltpu.CompilerParams(vmem_limit_bytes=24 * 1024 * 1024)


def dot(a, b, dims):
    return lax.dot_general(a, b, dims, preferred_element_type=F32)


def shift(x, axis, step):
    n = lax.axis_size(axis)
    return lax.ppermute(x, axis, [(i, i + step) for i in range(n) if 0 <= i + step < n])


def key_features(rows, cols, tr, tc):
    lane = np.arange(LANES)
    far_col = (lane < tc) & (np.abs(cols[..., None] - lane) > RADIUS)
    far_row = (lane >= tc) & (lane < tc + tr) & (np.abs(rows[..., None] - (lane - tc)) > RADIUS)
    return np.where(far_col | far_row, FAR, 0.0).astype(np.float32)


def query_features(rows, cols, tr, tc):
    lane = np.arange(LANES)
    hit = (lane == cols[..., None]) | (lane - tc == rows[..., None]) | (lane == tc + tr)
    return hit.astype(np.float32)


def with_grid_edge(const, off):
    lane = lax.broadcasted_iota(jnp.int32, const.shape, const.ndim - 1)
    return jnp.where((lane == off[1]) & off[0], FAR, jnp.asarray(const)).astype(BF16)


def copy_all(copies, sems):
    started = []
    for i, (src, dst) in enumerate(copies):
        c = pltpu.make_async_copy(src, dst, sems.at[i])
        c.start()
        started.append(c)
    return started


def pack_sides_kernel(p_ref, right_ref, left_ref, sems):
    tc = p_ref.shape[2]
    copies = []
    for j in range(2):
        copies.append((p_ref.at[1 + j, :, pl.ds(tc - RADIUS, RADIUS)], right_ref.at[j]))
        copies.append((p_ref.at[1 + j, :, pl.ds(0, RADIUS)], left_ref.at[j]))
    for c in copy_all(copies, sems):
        c.wait()


def pack_rows_kernel(p_ref, down_ref, up_ref, sems):
    _, tr, tc, _ = p_ref.shape
    copies = []
    for j in range(2):
        for g in range(tc // RADIUS):
            cols = pl.ds(g * RADIUS, RADIUS)
            copies.append((p_ref.at[1 + j, pl.ds(tr - RADIUS, RADIUS), cols], down_ref.at[j, g]))
            copies.append((p_ref.at[1 + j, pl.ds(0, RADIUS), cols], up_ref.at[j, g]))
    for c in copy_all(copies, sems):
        c.wait()


def pack(kernel, patches, shape, copies):
    payload = pltpu.VMEM(shape, BF16)
    return pl.pallas_call(
        kernel,
        in_specs=[HBM],
        out_specs=[VMEM] * 2,
        out_shape=[payload] * 2,
        scratch_shapes=[pltpu.SemaphoreType.DMA((copies,))],
        compiler_params=PARAMS,
    )(patches)


def prep_kernel(scale, flag_ref, reg_ref, p_ref, out_ref, part_ref, sems):
    _, tr, tc, width = p_ref.shape
    groups = tc // RADIUS
    count = reg_ref.shape[1]
    head = width // HEADS
    copies = [
        (p_ref.at[j, :, pl.ds(g * RADIUS, RADIUS)], out_ref.at[j, g])
        for j in (1, 2, 0)
        for g in range(groups)
    ]
    started = copy_all(copies, sems)
    lane_head = lax.broadcasted_iota(jnp.int32, (HEADS, count, width), 2) // head
    own = lane_head == lax.broadcasted_iota(jnp.int32, (HEADS, count, width), 0)
    q = reg_ref[0].astype(F32) * scale
    q = jnp.where(own, q[None], 0.0).reshape(HEADS * count, width).astype(BF16)
    self_scores = dot(reg_ref[1], q, NT) + flag_ref[0]
    for c in started[:groups]:
        c.wait()
    scores = dot(out_ref[1].reshape(tr * tc, width), q, NT)
    high = jnp.maximum(
        jnp.max(scores, axis=0, keepdims=True), jnp.max(self_scores, axis=0, keepdims=True)
    )
    w = jnp.exp(scores - high)
    self_w = jnp.exp(self_scores - high)
    total = jnp.sum(w, axis=0, keepdims=True) + jnp.sum(self_w, axis=0, keepdims=True)
    wt = jnp.transpose(w).astype(BF16)
    for c in started[groups:]:
        c.wait()
    acc = dot(wt, out_ref[2].reshape(tr * tc, width), NN)
    acc = acc + dot(jnp.transpose(self_w).astype(BF16), reg_ref[2], NN)
    acc = jnp.sum(jnp.where(own, acc.reshape(HEADS, count, width), 0.0), axis=0)
    n = HEADS * count

    def spread(row):
        col = jnp.transpose(jnp.broadcast_to(row, (LANES, n))).reshape(HEADS, count, LANES)
        low = lax.broadcasted_iota(jnp.int32, (count, LANES), 1) < head
        return jnp.concatenate(
            [jnp.where(low, col[2 * p], col[2 * p + 1]) for p in range(HEADS // 2)], axis=1
        )

    part_ref[0] = acc
    part_ref[1] = spread(high)
    part_ref[2] = spread(total)


def prep(patches, registers, flag, scale):
    _, tr, tc, width = patches.shape
    groups = tc // RADIUS
    count = registers.shape[1]
    return pl.pallas_call(
        functools.partial(prep_kernel, scale),
        in_specs=[SMEM, VMEM, HBM],
        out_specs=[VMEM, VMEM],
        out_shape=[
            pltpu.VMEM((3, groups, tr, RADIUS, width), BF16),
            pltpu.VMEM((3, count, width), F32),
        ],
        scratch_shapes=[pltpu.SemaphoreType.DMA((3 * groups,))],
        cost_estimate=pl.CostEstimate(
            flops=300_000_000, bytes_accessed=4_000_000, transcendentals=70_000
        ),
        compiler_params=PARAMS,
        name="prep",
    )(flag, registers, patches)


def merge(a, b):
    high = jnp.maximum(a[1], b[1])
    fa = jnp.exp(a[1] - high)
    fb = jnp.exp(b[1] - high)
    return jnp.stack([a[0] * fa + b[0] * fb, high, a[2] * fa + b[2] * fb])


def merge_over(part, axis):
    n = lax.axis_size(axis)
    if n & (n - 1):
        every = lax.all_gather(part, axis)
        return functools.reduce(merge, [every[i] for i in range(n)])
    step = 1
    while step < n:
        other = lax.ppermute(part, axis, [(i, i ^ step) for i in range(n)])
        part = merge(part, other)
        step *= 2
    return part


def centre_kernel(scale, first, p_ref, up_ref, down_ref, reg_ref, qf_ref, kf_ref, in_ref, st_ref):
    _, _, cells, width = p_ref.shape
    d = LANES
    head = width // HEADS
    edge = RADIUS * RADIUS
    low = lax.broadcasted_iota(jnp.int32, (edge, d), 1) < head
    pad = lax.broadcasted_iota(jnp.int32, (2 * RADIUS, d), 0) >= RADIUS
    off = lax.broadcasted_iota(jnp.int32, (2 * RADIUS, d), 1) == d - 1
    reg_f = jnp.where(pad & off, FAR, 0.0).astype(BF16)
    zero = jnp.zeros((RADIUS, d), BF16)

    @pl.loop(0, st_ref.shape[0])
    def _(i):
        lanes = pl.ds(pl.multiple_of((i + first) * d, d), d)
        lanes_out = pl.ds(pl.multiple_of(i * d, d), d)
        reg_k = jnp.concatenate([reg_ref[1, :, lanes], zero], axis=0)
        reg_v = jnp.concatenate([reg_ref[2, :, lanes], zero], axis=0)
        for half in range(2):
            for part in range(2):
                near = range(part, part + 3)

                def piece(j, g):
                    own = p_ref[1 + j, g, :, lanes]
                    if half == 0:
                        return [up_ref[j, g, :, lanes], own]
                    return [own, down_ref[j, g, :, lanes]]

                span = cells + edge
                k = jnp.concatenate(sum([piece(0, g) for g in near], []) + [reg_k], axis=0)
                v = jnp.concatenate(sum([piece(1, g) for g in near], []) + [reg_v], axis=0)
                f = jnp.concatenate(
                    [kf_ref[g, half * edge : half * edge + span] for g in near] + [reg_f], axis=0
                )
                kc = jnp.concatenate([k, f], axis=1)
                qs = []
                for g in (0, 1) if part == 0 else (3, 2):
                    rows = slice(half * edge, (half + 1) * edge)
                    q = p_ref[0, g, rows, lanes].astype(F32) * scale
                    qf = qf_ref[g, rows]
                    for x in (jnp.where(low, q, 0.0), jnp.where(low, 0.0, q)):
                        qs.append(jnp.concatenate([x.astype(BF16), qf], axis=1))
                s = dot(kc, jnp.concatenate(qs, axis=0), NT)
                high = jnp.max(s, axis=0, keepdims=True)
                w = jnp.exp(s - high)
                total = jnp.sum(w, axis=0, keepdims=True)
                o = dot(v, w.astype(BF16), TN)
                st_ref[i, half, part, :d] = o[:, :d]
                st_ref[i, half, part, d : d + 8] = jnp.concatenate(
                    [high[:, :d], total[:, :d], jnp.zeros((6, d), F32)], axis=0
                )
                t = jnp.transpose(o[:, d:] / total[:, d:])
                t = jnp.where(low, t[:edge], t[edge:])
                in_ref[part, half * edge : (half + 1) * edge, lanes_out] = t.astype(BF16)


def centre(pg, up, down, registers, qf, kf, scale, first, pairs):
    _, _, cells, _ = pg.shape
    edge = RADIUS * RADIUS
    d = LANES
    keys = 3 * (cells + edge) + 2 * RADIUS
    work = pairs * 4 * keys * 4 * edge
    return pl.pallas_call(
        functools.partial(centre_kernel, scale, first),
        in_specs=[VMEM] * 6,
        out_specs=[VMEM, VMEM],
        out_shape=[
            pltpu.VMEM((2, cells, pairs * d), BF16),
            pltpu.VMEM((pairs, 2, 2, d + 8, d), F32),
        ],
        cost_estimate=pl.CostEstimate(
            flops=work * 2 * 384, bytes_accessed=4_000_000, transcendentals=work
        ),
        compiler_params=PARAMS,
        name="centre",
    )(pg, up, down, registers, qf, kf)


def edge_kernel(
    scale, parts, p_ref, l_ref, r_ref, cu_ref, cd_ref, qf_ref, kf_ref, *refs
):
    inner, states = refs[:parts], refs[parts : 2 * parts]
    out_ref, edge_ref, sems = refs[2 * parts :]
    _, groups, cells, width = p_ref.shape
    d = LANES
    head = width // HEADS
    edge = RADIUS * RADIUS
    span = cells + edge
    low = lax.broadcasted_iota(jnp.int32, (edge, d), 1) < head
    per = states[0].shape[0]
    copies = []
    for n in range(parts):
        for part in range(2):
            g = 1 if part == 0 else groups - 2
            copies.append(
                (
                    inner[n].at[part],
                    out_ref.at[:, pl.ds(g * RADIUS, RADIUS), pl.ds(n * per * d, per * d)],
                )
            )
    started = copy_all(copies, sems)
    for n in range(parts):

        @pl.loop(0, per)
        def _(i):
            lanes = pl.ds(pl.multiple_of((i + n * per) * d, d), d)
            for half in range(2):
                cells_of = slice(half * edge, (half + 1) * edge)
                for side in range(2):
                    halo = l_ref if side == 0 else r_ref
                    corner = cu_ref if half == 0 else cd_ref

                    def keys(j):
                        own = halo[j, :, lanes]
                        far = corner[side, j, :, lanes]
                        return jnp.concatenate([far, own] if half == 0 else [own, far], axis=0)

                    f = kf_ref[side, half * edge : half * edge + span]
                    kc = jnp.concatenate([keys(0), f], axis=1)
                    g = 0 if side == 0 else groups - 1
                    q = p_ref[0, g, cells_of, lanes].astype(F32) * scale
                    qf = qf_ref[g, cells_of]
                    qc = jnp.concatenate(
                        [
                            jnp.concatenate([x.astype(BF16), qf], axis=1)
                            for x in (jnp.where(low, q, 0.0), jnp.where(low, 0.0, q))
                        ],
                        axis=0,
                    )
                    s = dot(kc, qc, NT)
                    st = states[n]
                    high1 = st[i, half, side, d : d + 1]
                    total1 = st[i, half, side, d + 1 : d + 2]
                    high = jnp.maximum(high1, jnp.max(s, axis=0, keepdims=True))
                    fade = jnp.exp(high1 - high)
                    w = jnp.exp(s - high)
                    total = total1 * fade + jnp.sum(w, axis=0, keepdims=True)
                    acc = st[i, half, side, :d] * fade + dot(keys(1), w.astype(BF16), TN)
                    t = jnp.transpose(acc / total)
                    t = jnp.where(low, t[:edge], t[edge:])
                    rows_of = slice(half * RADIUS, (half + 1) * RADIUS)
                    edge_ref[side, rows_of, :, lanes] = t.reshape(RADIUS, RADIUS, d).astype(BF16)

    copies = []
    for side in range(2):
        g = 0 if side == 0 else groups - 1
        copies.append(
            (edge_ref.at[side], out_ref.at[:, pl.ds(g * RADIUS, RADIUS)])
        )
    started += copy_all(copies, sems.at[pl.ds(2 * parts, 2)])
    for c in started:
        c.wait()


def edges(pg, left, right, corner_up, corner_down, qf, kf, inner, states, scale, tr, tc):
    _, _, _, width = pg.shape
    parts = len(states)
    return pl.pallas_call(
        functools.partial(edge_kernel, scale, parts),
        in_specs=[VMEM] * (7 + 2 * parts),
        out_specs=HBM,
        out_shape=jax.ShapeDtypeStruct((tr, tc, width), BF16),
        scratch_shapes=[
            pltpu.VMEM((2, tr, RADIUS, width), BF16),
            pltpu.SemaphoreType.DMA((2 * parts + 2,)),
        ],
        cost_estimate=pl.CostEstimate(
            flops=500_000_000, bytes_accessed=3_000_000, transcendentals=800_000
        ),
        compiler_params=PARAMS,
        name="edges",
    )(pg, left, right, corner_up, corner_down, qf, kf, *inner, *states)


def local(patches, registers):
    _, tr, tc, width = patches.shape
    groups = tc // RADIUS
    cells = tr * RADIUS
    edge = RADIUS * RADIUS
    assert tr == 2 * RADIUS and groups == 4 and 2 * width == HEADS * LANES
    scale = (width // HEADS) ** (-0.5)
    row_at, row_n = lax.axis_index("row"), lax.axis_size("row")
    col_at, col_n = lax.axis_index("col"), lax.axis_size("col")

    source = pltpu.with_memory_space_constraint(patches, pltpu.HBM)
    to_right, to_left = pack(pack_sides_kernel, source, (2, tr, RADIUS, width), 4)
    left = shift(to_right, "col", 1)
    right = shift(to_left, "col", -1)
    shape = (2, groups, RADIUS, RADIUS, width)
    to_down, to_up = pack(pack_rows_kernel, source, shape, 4 * groups)
    up = shift(to_down, "row", 1)
    down = shift(to_up, "row", -1)
    left, right = (x.reshape(2, cells, width) for x in (left, right))
    up, down = (x.reshape(2, groups, edge, width) for x in (up, down))

    flag = jnp.where((row_at == 0) & (col_at == 0), 0.0, -1e30).astype(F32).reshape(1)
    pg, part = prep(source, registers, flag, scale)
    pg = pg.reshape(3, groups, cells, width)
    part = merge_over(merge_over(part, "row"), "col")
    register_out = (part[0] / part[2]).astype(BF16)

    key_rows = np.repeat(np.arange(-RADIUS, tr + RADIUS), RADIUS)
    key_cols = np.tile(np.arange(RADIUS), tr + 2 * RADIUS)
    stack = lambda cols: np.stack([key_features(key_rows, key_cols + c, tr, tc) for c in cols])
    row = jnp.arange((tr + 2 * RADIUS) * RADIUS, dtype=jnp.int32)[None, :, None]
    off_rows = ((row < edge) & (row_at == 0)) | ((row >= edge + cells) & (row_at == row_n - 1))
    side = jnp.arange(2, dtype=jnp.int32)[:, None, None]
    off_cols = ((side == 0) & (col_at == 0)) | ((side == 1) & (col_at == col_n - 1))
    off_lane = LANES - 1
    kf = with_grid_edge(stack([g * RADIUS for g in range(groups)]), (off_rows, off_lane))
    kf_side = with_grid_edge(stack([-RADIUS, tc]), (off_rows | off_cols, off_lane))
    q_rows = np.repeat(np.arange(tr), RADIUS)
    q_cols = np.tile(np.arange(RADIUS), tr)
    qf = np.stack([query_features(q_rows, q_cols + g * RADIUS, tr, tc) for g in range(groups)])
    qf[..., off_lane] = 1.0
    qf = jnp.asarray(qf.astype(BF16))

    pairs = HEADS // 2
    parts = PARTS
    per = pairs // parts
    done = []
    for n in range(parts):
        done.append(centre(pg, up, down, registers, qf, kf, scale, n * per, per))
    near_l, near_r, first_state = lax.optimization_barrier((left, right, done[0][1]))
    done[0] = (done[0][0], first_state)
    bottom = jnp.stack([near_l[:, -edge:], near_r[:, -edge:]])
    corner_up = shift(bottom, "row", 1)
    top = jnp.stack([near_l[:, :edge], near_r[:, :edge]])
    corner_down = shift(top, "row", -1)
    inner = [x[0].reshape(2, tr, RADIUS, per * LANES) for x in done]
    out = edges(
        pg, left, right, corner_up, corner_down, qf, kf_side, inner, [x[1] for x in done], scale, tr, tc
    )
    return (out, register_out)


def solution(mesh):
    in_specs = (P(None, "row", "col", None), P())
    out_specs = (P("row", "col", None), P())
    return jax.shard_map(local, mesh=mesh, in_specs=in_specs, out_specs=out_specs, check_vma=False)
```

```python
import functools

import jax
import jax.numpy as jnp
import numpy as np
from jax import lax
from jax.experimental import pallas as pl
from jax.experimental.pallas import tpu as pltpu
from jax.sharding import PartitionSpec as P


HEADS = 16
PARTS = 4
RADIUS = 8
FAR = -30000.0
LEAST, MOST = 1e-20, 1e30
LANES = 128
F32 = jnp.float32
BF16 = jnp.bfloat16
NT = (((1,), (1,)), ((), ()))
NN = (((1,), (0,)), ((), ()))
TN = (((0,), (0,)), ((), ()))
VMEM = pl.BlockSpec(memory_space=pltpu.VMEM)
HBM = pl.BlockSpec(memory_space=pltpu.HBM)
SMEM = pl.BlockSpec(memory_space=pltpu.SMEM)
PARAMS = pltpu.CompilerParams(vmem_limit_bytes=24 * 1024 * 1024)


def dot(a, b, dims):
    return lax.dot_general(a, b, dims, preferred_element_type=F32)


def shift(x, axis, step):
    n = lax.axis_size(axis)
    return lax.ppermute(x, axis, [(i, i + step) for i in range(n) if 0 <= i + step < n])


def key_features(rows, cols, tr, tc):
    lane = np.arange(LANES)
    far_col = (lane < tc) & (np.abs(cols[..., None] - lane) > RADIUS)
    far_row = (lane >= tc) & (lane < tc + tr) & (np.abs(rows[..., None] - (lane - tc)) > RADIUS)
    return np.where(far_col | far_row, FAR, 0.0).astype(np.float32)


def query_features(rows, cols, tr, tc):
    lane = np.arange(LANES)
    hit = (lane == cols[..., None]) | (lane - tc == rows[..., None]) | (lane == tc + tr)
    return hit.astype(np.float32)


def with_grid_edge(const, off):
    lane = lax.broadcasted_iota(jnp.int32, const.shape, const.ndim - 1)
    return jnp.where((lane == off[1]) & off[0], FAR, jnp.asarray(const)).astype(BF16)


def copy_all(copies, sems):
    started = []
    for i, (src, dst) in enumerate(copies):
        c = pltpu.make_async_copy(src, dst, sems.at[i])
        c.start()
        started.append(c)
    return started


def stage_kernel(copies_of, a_ref, b_ref, a_out, b_out, sems):
    copies = copies_of(a_ref, a_out) + copies_of(b_ref, b_out)
    for c in copy_all(copies, sems):
        c.wait()


def whole(src, dst):
    return [(src.at[j], dst.at[j]) for j in range(2)]


def grouped(src, dst):
    cut = lambda g: pl.ds(g * RADIUS, RADIUS)
    return [(src.at[j, :, cut(g)], dst.at[j, g]) for j in range(2) for g in range(dst.shape[1])]


def stage(copies_of, count, a, b, shape):
    a, b = (pltpu.with_memory_space_constraint(x, pltpu.HBM) for x in (a, b))
    return pl.pallas_call(
        functools.partial(stage_kernel, copies_of),
        in_specs=[HBM, HBM],
        out_specs=[VMEM, VMEM],
        out_shape=[pltpu.VMEM(shape, BF16)] * 2,
        scratch_shapes=[pltpu.SemaphoreType.DMA((2 * count,))],
        cost_estimate=pl.CostEstimate(flops=1_000_000, bytes_accessed=4_000_000, transcendentals=0),
        compiler_params=PARAMS,
    )(a, b)


def prep_kernel(scale, flag_ref, reg_ref, p_ref, out_ref, part_ref, sems):
    _, tr, tc, width = p_ref.shape
    groups = tc // RADIUS
    count = reg_ref.shape[1]
    head = width // HEADS
    copies = [
        (p_ref.at[j, :, pl.ds(g * RADIUS, RADIUS)], out_ref.at[j, g])
        for j in (1, 2, 0)
        for g in range(groups)
    ]
    started = copy_all(copies, sems)
    lane_head = lax.broadcasted_iota(jnp.int32, (HEADS, count, width), 2) // head
    own = lane_head == lax.broadcasted_iota(jnp.int32, (HEADS, count, width), 0)
    q = reg_ref[0].astype(F32) * scale
    q = jnp.where(own, q[None], 0.0).reshape(HEADS * count, width).astype(BF16)
    self_scores = dot(reg_ref[1], q, NT) + flag_ref[0]
    for c in started[:groups]:
        c.wait()
    scores = dot(out_ref[1].reshape(tr * tc, width), q, NT)
    high = jnp.maximum(
        jnp.max(scores, axis=0, keepdims=True), jnp.max(self_scores, axis=0, keepdims=True)
    )
    w = jnp.exp(scores - high)
    self_w = jnp.exp(self_scores - high)
    total = jnp.sum(w, axis=0, keepdims=True) + jnp.sum(self_w, axis=0, keepdims=True)
    wt = jnp.transpose(w).astype(BF16)
    for c in started[groups:]:
        c.wait()
    acc = dot(wt, out_ref[2].reshape(tr * tc, width), NN)
    acc = acc + dot(jnp.transpose(self_w).astype(BF16), reg_ref[2], NN)
    acc = jnp.sum(jnp.where(own, acc.reshape(HEADS, count, width), 0.0), axis=0)
    n = HEADS * count

    def spread(row):
        col = jnp.transpose(jnp.broadcast_to(row, (LANES, n))).reshape(HEADS, count, LANES)
        low = lax.broadcasted_iota(jnp.int32, (count, LANES), 1) < head
        return jnp.concatenate(
            [jnp.where(low, col[2 * p], col[2 * p + 1]) for p in range(HEADS // 2)], axis=1
        )

    part_ref[0] = acc
    part_ref[1] = spread(high)
    part_ref[2] = spread(total)


def prep(patches, registers, flag, scale):
    _, tr, tc, width = patches.shape
    groups = tc // RADIUS
    count = registers.shape[1]
    return pl.pallas_call(
        functools.partial(prep_kernel, scale),
        in_specs=[SMEM, VMEM, HBM],
        out_specs=[VMEM, VMEM],
        out_shape=[
            pltpu.VMEM((3, groups, tr, RADIUS, width), BF16),
            pltpu.VMEM((3, count, width), F32),
        ],
        scratch_shapes=[pltpu.SemaphoreType.DMA((3 * groups,))],
        cost_estimate=pl.CostEstimate(
            flops=300_000_000, bytes_accessed=4_000_000, transcendentals=70_000
        ),
        compiler_params=PARAMS,
        name="prep",
    )(flag, registers, patches)


def merge(a, b):
    high = jnp.maximum(a[1], b[1])
    fa = jnp.exp(a[1] - high)
    fb = jnp.exp(b[1] - high)
    return jnp.stack([a[0] * fa + b[0] * fb, high, a[2] * fa + b[2] * fb])


def merge_over(part, axis):
    n = lax.axis_size(axis)
    if n & (n - 1):
        every = lax.all_gather(part, axis)
        return functools.reduce(merge, [every[i] for i in range(n)])
    step = 1
    while step < n:
        other = lax.ppermute(part, axis, [(i, i ^ step) for i in range(n)])
        part = merge(part, other)
        step *= 2
    return part


def centre_kernel(scale, first, p_ref, up_ref, down_ref, reg_ref, qf_ref, kf_ref, in_ref, st_ref):
    _, groups, cells, width = p_ref.shape
    d = LANES
    head = width // HEADS
    edge = RADIUS * RADIUS
    low = lax.broadcasted_iota(jnp.int32, (edge, d), 1) < head
    pad = lax.broadcasted_iota(jnp.int32, (2 * RADIUS, d), 0) >= RADIUS
    off = lax.broadcasted_iota(jnp.int32, (2 * RADIUS, d), 1) == d - 1
    reg_f = jnp.where(pad & off, FAR, 0.0).astype(BF16)
    zero = jnp.zeros((RADIUS, d), BF16)

    def unit(i, half, part, exact):
        lanes = pl.ds(pl.multiple_of((i + first) * d, d), d)
        lanes_out = pl.ds(pl.multiple_of(i * d, d), d)
        rows = slice(half * edge, (half + 1) * edge)
        near = range(part, part + 3)
        span = cells + edge

        def stacked(j):
            pieces = []
            for g in near:
                own = p_ref[j, g, :, lanes]
                if half == 0:
                    pieces += [up_ref[j - 1, g, :, lanes], own]
                else:
                    pieces += [own, down_ref[j - 1, g, :, lanes]]
            return jnp.concatenate(pieces + [reg_ref[j, :, lanes], zero], axis=0)

        f = jnp.concatenate(
            [kf_ref[g, half * edge : half * edge + span] for g in near] + [reg_f], axis=0
        )
        kc = jnp.concatenate([stacked(1), f], axis=1)
        qs = []
        for g in (0, 1) if part == 0 else (groups - 1, groups - 2):
            q = p_ref[0, g, rows, lanes].astype(F32) * scale
            qf = qf_ref[g, rows]
            for x in (jnp.where(low, q, 0.0), jnp.where(low, 0.0, q)):
                qs.append(jnp.concatenate([x.astype(BF16), qf], axis=1))
        s = dot(kc, jnp.concatenate(qs, axis=0), NT)
        if exact:
            high = jnp.max(s, axis=0, keepdims=True)
            s = s - high
        else:
            high = jnp.zeros((1, s.shape[1]), F32)
        w = jnp.exp(s)
        total = jnp.sum(w, axis=0, keepdims=True)
        o = dot(stacked(2), w.astype(BF16), TN)
        st_ref[i, half, part, :d] = o[:, :d]
        st_ref[i, half, part, d : d + 8] = jnp.concatenate(
            [high[:, :d], total[:, :d], jnp.zeros((6, d), F32)], axis=0
        )
        t = jnp.transpose(o[:, d:] / total[:, d:])
        t = jnp.where(low, t[:edge], t[edge:])
        in_ref[part, rows, lanes_out] = t.astype(BF16)
        return total

    run_guarded(unit, st_ref.shape[0], 4 * edge)


def run_guarded(unit, count, lanes):
    units = [(half, part) for half in range(2) for part in range(2)]

    def fast(i, seen):
        least, most = seen
        for half, part in units:
            total = unit(i, half, part, False)
            least = jnp.where(total >= least, least, total)
            most = jnp.where(total <= most, most, total)
        return least, most

    one = jnp.ones((1, lanes), F32)
    least, most = lax.fori_loop(0, count, fast, (one, one))
    fine = jnp.where((least > LEAST) & (most < MOST), 1.0, 0.0)

    @pl.when(jnp.min(fine) < 0.5)
    def _():
        @pl.loop(0, count)
        def _(i):
            for half, part in units:
                unit(i, half, part, True)


def centre(pg, up, down, registers, qf, kf, scale, first, pairs):
    _, _, cells, _ = pg.shape
    edge = RADIUS * RADIUS
    d = LANES
    keys = 3 * (cells + edge) + 2 * RADIUS
    work = pairs * 4 * keys * 4 * edge
    return pl.pallas_call(
        functools.partial(centre_kernel, scale, first),
        in_specs=[VMEM] * 6,
        out_specs=[VMEM, VMEM],
        out_shape=[
            pltpu.VMEM((2, cells, pairs * d), BF16),
            pltpu.VMEM((pairs, 2, 2, d + 8, d), F32),
        ],
        cost_estimate=pl.CostEstimate(
            flops=work * 2 * 384, bytes_accessed=4_000_000, transcendentals=work
        ),
        compiler_params=PARAMS,
        name="centre",
    )(pg, up, down, registers, qf, kf)


def edge_kernel(
    scale, parts, p_ref, l_ref, r_ref, cu_ref, cd_ref, qf_ref, kf_ref, *refs
):
    inner, states = refs[:parts], refs[parts : 2 * parts]
    out_ref, edge_ref, sems = refs[2 * parts :]
    _, groups, cells, width = p_ref.shape
    d = LANES
    head = width // HEADS
    edge = RADIUS * RADIUS
    span = cells + edge
    low = lax.broadcasted_iota(jnp.int32, (edge, d), 1) < head
    per = states[0].shape[0]
    copies = []
    for n in range(parts):
        for part in range(2):
            g = 1 if part == 0 else groups - 2
            copies.append(
                (
                    inner[n].at[part],
                    out_ref.at[:, pl.ds(g * RADIUS, RADIUS), pl.ds(n * per * d, per * d)],
                )
            )
    started = copy_all(copies, sems)

    def unit_of(n, i, half, side, exact):
        st = states[n]
        lanes = pl.ds(pl.multiple_of((i + n * per) * d, d), d)
        cells_of = slice(half * edge, (half + 1) * edge)
        halo = l_ref if side == 0 else r_ref
        corner = cu_ref if half == 0 else cd_ref

        def keys(j):
            own = halo[j, :, lanes]
            far = corner[side, j, :, lanes]
            return jnp.concatenate([far, own] if half == 0 else [own, far], axis=0)

        f = kf_ref[side, half * edge : half * edge + span]
        kc = jnp.concatenate([keys(0), f], axis=1)
        g = 0 if side == 0 else groups - 1
        q = p_ref[0, g, cells_of, lanes].astype(F32) * scale
        qf = qf_ref[g, cells_of]
        qc = jnp.concatenate(
            [
                jnp.concatenate([x.astype(BF16), qf], axis=1)
                for x in (jnp.where(low, q, 0.0), jnp.where(low, 0.0, q))
            ],
            axis=0,
        )
        s = dot(kc, qc, NT)
        acc = st[i, half, side, :d]
        high = st[i, half, side, d : d + 1]
        total = st[i, half, side, d + 1 : d + 2]
        if exact:
            new = jnp.maximum(high, jnp.max(s, axis=0, keepdims=True))
            fade = jnp.exp(high - new)
            acc, total, high = acc * fade, total * fade, new
        w = jnp.exp(s - high)
        total = total + jnp.sum(w, axis=0, keepdims=True)
        acc = acc + dot(keys(1), w.astype(BF16), TN)
        t = jnp.transpose(acc / total)
        t = jnp.where(low, t[:edge], t[edge:])
        rows_of = slice(half * RADIUS, (half + 1) * RADIUS)
        edge_ref[side, rows_of, :, lanes] = t.reshape(RADIUS, RADIUS, d).astype(BF16)
        return total

    for n in range(parts):
        run_guarded(functools.partial(unit_of, n), per, 2 * edge)

    copies = []
    for side in range(2):
        g = 0 if side == 0 else groups - 1
        copies.append(
            (edge_ref.at[side], out_ref.at[:, pl.ds(g * RADIUS, RADIUS)])
        )
    started += copy_all(copies, sems.at[pl.ds(2 * parts, 2)])
    for c in started:
        c.wait()


def edges(pg, left, right, corner_up, corner_down, qf, kf, inner, states, scale, tr, tc):
    _, _, _, width = pg.shape
    parts = len(states)
    return pl.pallas_call(
        functools.partial(edge_kernel, scale, parts),
        in_specs=[VMEM] * (7 + 2 * parts),
        out_specs=HBM,
        out_shape=jax.ShapeDtypeStruct((tr, tc, width), BF16),
        scratch_shapes=[
            pltpu.VMEM((2, tr, RADIUS, width), BF16),
            pltpu.SemaphoreType.DMA((2 * parts + 2,)),
        ],
        cost_estimate=pl.CostEstimate(
            flops=500_000_000, bytes_accessed=3_000_000, transcendentals=800_000
        ),
        compiler_params=PARAMS,
        name="edges",
    )(pg, left, right, corner_up, corner_down, qf, kf, *inner, *states)


def local(patches, registers):
    _, tr, tc, width = patches.shape
    groups = tc // RADIUS
    cells = tr * RADIUS
    edge = RADIUS * RADIUS
    assert tr == 2 * RADIUS and groups == 4 and 2 * width == HEADS * LANES
    scale = (width // HEADS) ** (-0.5)
    row_at, row_n = lax.axis_index("row"), lax.axis_size("row")
    col_at, col_n = lax.axis_index("col"), lax.axis_size("col")

    in_vmem = lambda x: pltpu.with_memory_space_constraint(x, pltpu.VMEM)
    source = pltpu.with_memory_space_constraint(patches, pltpu.HBM)
    left = shift(patches[1:3, :, tc - RADIUS :], "col", 1)
    right = shift(patches[1:3, :, :RADIUS], "col", -1)
    up = shift(patches[1:3, tr - RADIUS :], "row", 1)
    down = shift(patches[1:3, :RADIUS], "row", -1)
    left, right = (x.reshape(2, cells, width) for x in (left, right))
    rows_shape = (2, groups, RADIUS, RADIUS, width)
    up, down = stage(grouped, 2 * groups, up, down, rows_shape)
    up, down = (x.reshape(2, groups, edge, width) for x in (up, down))

    flag = jnp.where((row_at == 0) & (col_at == 0), 0.0, -1e30).astype(F32).reshape(1)
    pg, part = prep(source, registers, flag, scale)
    pg = pg.reshape(3, groups, cells, width)
    part = merge_over(merge_over(part, "row"), "col")
    register_out = (part[0] / part[2]).astype(BF16)

    key_rows = np.repeat(np.arange(-RADIUS, tr + RADIUS), RADIUS)
    key_cols = np.tile(np.arange(RADIUS), tr + 2 * RADIUS)
    stack = lambda cols: np.stack([key_features(key_rows, key_cols + c, tr, tc) for c in cols])
    row = jnp.arange((tr + 2 * RADIUS) * RADIUS, dtype=jnp.int32)[None, :, None]
    off_rows = ((row < edge) & (row_at == 0)) | ((row >= edge + cells) & (row_at == row_n - 1))
    side = jnp.arange(2, dtype=jnp.int32)[:, None, None]
    off_cols = ((side == 0) & (col_at == 0)) | ((side == 1) & (col_at == col_n - 1))
    off_lane = LANES - 1
    kf = with_grid_edge(stack([g * RADIUS for g in range(groups)]), (off_rows, off_lane))
    kf_side = with_grid_edge(stack([-RADIUS, tc]), (off_rows | off_cols, off_lane))
    q_rows = np.repeat(np.arange(tr), RADIUS)
    q_cols = np.tile(np.arange(RADIUS), tr)
    qf = np.stack([query_features(q_rows, q_cols + g * RADIUS, tr, tc) for g in range(groups)])
    qf[..., off_lane] = 1.0
    qf = jnp.asarray(qf.astype(BF16))

    pairs = HEADS // 2
    parts = PARTS
    per = pairs // parts
    done = []
    for n in range(parts):
        done.append(centre(pg, up, down, registers, qf, kf, scale, n * per, per))
    near_l, near_r, first_state = lax.optimization_barrier((left, right, done[0][1]))
    done[0] = (done[0][0], first_state)
    bottom = jnp.stack([near_l[:, -edge:], near_r[:, -edge:]])
    corner_up = in_vmem(shift(bottom, "row", 1))
    top = jnp.stack([near_l[:, :edge], near_r[:, :edge]])
    corner_down = in_vmem(shift(top, "row", -1))
    left, right = stage(whole, 2, near_l, near_r, left.shape)
    inner = [x[0].reshape(2, tr, RADIUS, per * LANES) for x in done]
    out = edges(
        pg, left, right, corner_up, corner_down, qf, kf_side, inner, [x[1] for x in done], scale, tr, tc
    )
    return (out, register_out)


def solution(mesh):
    in_specs = (P(None, "row", "col", None), P())
    out_specs = (P("row", "col", None), P())
    return jax.shard_map(local, mesh=mesh, in_specs=in_specs, out_specs=out_specs, check_vma=False)
```

```python
import functools

import jax
import jax.numpy as jnp
import numpy as np
from jax import lax
from jax.experimental import pallas as pl
from jax.experimental.pallas import tpu as pltpu
from jax.sharding import PartitionSpec as P


HEADS = 16
PARTS = 4
TOGETHER_C = 2
TOGETHER_E = 2
RADIUS = 8
FAR = -30000.0
LEAST, MOST = 1e-20, 1e30
LANES = 128
F32 = jnp.float32
BF16 = jnp.bfloat16
NT = (((1,), (1,)), ((), ()))
NN = (((1,), (0,)), ((), ()))
TN = (((0,), (0,)), ((), ()))
VMEM = pl.BlockSpec(memory_space=pltpu.VMEM)
HBM = pl.BlockSpec(memory_space=pltpu.HBM)
SMEM = pl.BlockSpec(memory_space=pltpu.SMEM)
PARAMS = pltpu.CompilerParams(vmem_limit_bytes=24 * 1024 * 1024)


def dot(a, b, dims):
    return lax.dot_general(a, b, dims, preferred_element_type=F32)


def shift(x, axis, step):
    n = lax.axis_size(axis)
    return lax.ppermute(x, axis, [(i, i + step) for i in range(n) if 0 <= i + step < n])


def key_features(rows, cols, tr, tc):
    lane = np.arange(LANES)
    far_col = (lane < tc) & (np.abs(cols[..., None] - lane) > RADIUS)
    far_row = (lane >= tc) & (lane < tc + tr) & (np.abs(rows[..., None] - (lane - tc)) > RADIUS)
    return np.where(far_col | far_row, FAR, 0.0).astype(np.float32)


def query_features(rows, cols, tr, tc):
    lane = np.arange(LANES)
    hit = (lane == cols[..., None]) | (lane - tc == rows[..., None]) | (lane == tc + tr)
    return hit.astype(np.float32)


def with_grid_edge(const, off):
    lane = lax.broadcasted_iota(jnp.int32, const.shape, const.ndim - 1)
    return jnp.where((lane == off[1]) & off[0], FAR, jnp.asarray(const)).astype(BF16)


def copy_all(copies, sems):
    started = []
    for i, (src, dst) in enumerate(copies):
        c = pltpu.make_async_copy(src, dst, sems.at[i])
        c.start()
        started.append(c)
    return started


def stage_kernel(copies_of, a_ref, b_ref, a_out, b_out, sems):
    copies = copies_of(a_ref, a_out) + copies_of(b_ref, b_out)
    for c in copy_all(copies, sems):
        c.wait()


def whole(src, dst):
    return [(src.at[j], dst.at[j]) for j in range(2)]


def grouped(src, dst):
    cut = lambda g: pl.ds(g * RADIUS, RADIUS)
    return [(src.at[j, :, cut(g)], dst.at[j, g]) for j in range(2) for g in range(dst.shape[1])]


def stage(copies_of, count, a, b, shape):
    a, b = (pltpu.with_memory_space_constraint(x, pltpu.HBM) for x in (a, b))
    return pl.pallas_call(
        functools.partial(stage_kernel, copies_of),
        in_specs=[HBM, HBM],
        out_specs=[VMEM, VMEM],
        out_shape=[pltpu.VMEM(shape, BF16)] * 2,
        scratch_shapes=[pltpu.SemaphoreType.DMA((2 * count,))],
        cost_estimate=pl.CostEstimate(flops=1_000_000, bytes_accessed=4_000_000, transcendentals=0),
        compiler_params=PARAMS,
    )(a, b)


def prep_kernel(scale, flag_ref, reg_ref, p_ref, out_ref, part_ref, sems):
    _, tr, tc, width = p_ref.shape
    groups = tc // RADIUS
    count = reg_ref.shape[1]
    head = width // HEADS
    copies = [
        (p_ref.at[j, :, pl.ds(g * RADIUS, RADIUS)], out_ref.at[j, g])
        for j in (1, 2, 0)
        for g in range(groups)
    ]
    started = copy_all(copies, sems)
    lane_head = lax.broadcasted_iota(jnp.int32, (HEADS, count, width), 2) // head
    own = lane_head == lax.broadcasted_iota(jnp.int32, (HEADS, count, width), 0)
    q = reg_ref[0].astype(F32) * scale
    q = jnp.where(own, q[None], 0.0).reshape(HEADS * count, width).astype(BF16)
    self_scores = dot(reg_ref[1], q, NT) + flag_ref[0]
    for c in started[:groups]:
        c.wait()
    scores = dot(out_ref[1].reshape(tr * tc, width), q, NT)
    high = jnp.maximum(
        jnp.max(scores, axis=0, keepdims=True), jnp.max(self_scores, axis=0, keepdims=True)
    )
    w = jnp.exp(scores - high)
    self_w = jnp.exp(self_scores - high)
    total = jnp.sum(w, axis=0, keepdims=True) + jnp.sum(self_w, axis=0, keepdims=True)
    wt = jnp.transpose(w).astype(BF16)
    for c in started[groups:]:
        c.wait()
    acc = dot(wt, out_ref[2].reshape(tr * tc, width), NN)
    acc = acc + dot(jnp.transpose(self_w).astype(BF16), reg_ref[2], NN)
    acc = jnp.sum(jnp.where(own, acc.reshape(HEADS, count, width), 0.0), axis=0)
    n = HEADS * count

    def spread(row):
        col = jnp.transpose(jnp.broadcast_to(row, (LANES, n))).reshape(HEADS, count, LANES)
        low = lax.broadcasted_iota(jnp.int32, (count, LANES), 1) < head
        return jnp.concatenate(
            [jnp.where(low, col[2 * p], col[2 * p + 1]) for p in range(HEADS // 2)], axis=1
        )

    part_ref[0] = acc
    part_ref[1] = spread(high)
    part_ref[2] = spread(total)


def prep(patches, registers, flag, scale):
    _, tr, tc, width = patches.shape
    groups = tc // RADIUS
    count = registers.shape[1]
    return pl.pallas_call(
        functools.partial(prep_kernel, scale),
        in_specs=[SMEM, VMEM, HBM],
        out_specs=[VMEM, VMEM],
        out_shape=[
            pltpu.VMEM((3, groups, tr, RADIUS, width), BF16),
            pltpu.VMEM((3, count, width), F32),
        ],
        scratch_shapes=[pltpu.SemaphoreType.DMA((3 * groups,))],
        cost_estimate=pl.CostEstimate(
            flops=300_000_000, bytes_accessed=4_000_000, transcendentals=70_000
        ),
        compiler_params=PARAMS,
        name="prep",
    )(flag, registers, patches)


def merge(a, b):
    high = jnp.maximum(a[1], b[1])
    fa = jnp.exp(a[1] - high)
    fb = jnp.exp(b[1] - high)
    return jnp.stack([a[0] * fa + b[0] * fb, high, a[2] * fa + b[2] * fb])


def merge_over(part, axis):
    n = lax.axis_size(axis)
    if n & (n - 1):
        every = lax.all_gather(part, axis)
        return functools.reduce(merge, [every[i] for i in range(n)])
    step = 1
    while step < n:
        other = lax.ppermute(part, axis, [(i, i ^ step) for i in range(n)])
        part = merge(part, other)
        step *= 2
    return part


def centre_kernel(scale, first, p_ref, up_ref, down_ref, reg_ref, qf_ref, kf_ref, in_ref, st_ref):
    _, groups, cells, width = p_ref.shape
    d = LANES
    head = width // HEADS
    edge = RADIUS * RADIUS
    low = lax.broadcasted_iota(jnp.int32, (edge, d), 1) < head
    pad = lax.broadcasted_iota(jnp.int32, (2 * RADIUS, d), 0) >= RADIUS
    off = lax.broadcasted_iota(jnp.int32, (2 * RADIUS, d), 1) == d - 1
    reg_f = jnp.where(pad & off, FAR, 0.0).astype(BF16)
    zero = jnp.zeros((RADIUS, d), BF16)

    def unit(i, half, part, exact):
        lanes = pl.ds(pl.multiple_of((i + first) * d, d), d)
        lanes_out = pl.ds(pl.multiple_of(i * d, d), d)
        rows = slice(half * edge, (half + 1) * edge)
        near = range(part, part + 3)
        span = cells + edge

        def stacked(j):
            pieces = []
            for g in near:
                own = p_ref[j, g, :, lanes]
                if half == 0:
                    pieces += [up_ref[j - 1, g, :, lanes], own]
                else:
                    pieces += [own, down_ref[j - 1, g, :, lanes]]
            return jnp.concatenate(pieces + [reg_ref[j, :, lanes], zero], axis=0)

        f = jnp.concatenate(
            [kf_ref[g, half * edge : half * edge + span] for g in near] + [reg_f], axis=0
        )
        kc = jnp.concatenate([stacked(1), f], axis=1)
        qs = []
        for g in (0, 1) if part == 0 else (groups - 1, groups - 2):
            q = p_ref[0, g, rows, lanes].astype(F32) * scale
            qf = qf_ref[g, rows]
            for x in (jnp.where(low, q, 0.0), jnp.where(low, 0.0, q)):
                qs.append(jnp.concatenate([x.astype(BF16), qf], axis=1))
        s = dot(kc, jnp.concatenate(qs, axis=0), NT)
        if exact:
            high = jnp.max(s, axis=0, keepdims=True)
            s = s - high
        else:
            high = jnp.zeros((1, s.shape[1]), F32)
        w = jnp.exp(s).astype(BF16)
        total = jnp.sum(w.astype(F32), axis=0, keepdims=True)
        yield total
        o = dot(stacked(2), w, TN)
        st_ref[i, half, part, :d] = o[:, :d]
        st_ref[i, half, part, d : d + 8] = jnp.concatenate(
            [high[:, :d], total[:, :d], jnp.zeros((6, d), F32)], axis=0
        )
        t = jnp.transpose(o[:, d:] / total[:, d:])
        t = jnp.where(low, t[:edge], t[edge:])
        in_ref[part, rows, lanes_out] = t.astype(BF16)

    run_guarded(unit, st_ref.shape[0], 4 * edge, TOGETHER_C)


def run_guarded(unit, count, lanes, together=1):
    units = [(half, part) for half in range(2) for part in range(2)]

    def both(i, exact):
        step = 1 if exact else together
        running = [
            unit(i * step + k, half, part, exact) for k in range(step) for half, part in units
        ]
        totals = [next(r) for r in running]
        for r in running:
            next(r, None)
        return totals

    def fast(i, seen):
        least, most = seen
        for total in both(i, False):
            least = jnp.where(total >= least, least, total)
            most = jnp.where(total <= most, most, total)
        return least, most

    one = jnp.ones((1, lanes), F32)
    least, most = lax.fori_loop(0, count // together, fast, (one, one))
    fine = jnp.where((least > LEAST) & (most < MOST), 1.0, 0.0)

    @pl.when(jnp.min(fine) < 0.5)
    def _():
        @pl.loop(0, count)
        def _(i):
            both(i, True)


def centre(pg, up, down, registers, qf, kf, scale, first, pairs):
    _, _, cells, _ = pg.shape
    edge = RADIUS * RADIUS
    d = LANES
    keys = 3 * (cells + edge) + 2 * RADIUS
    work = pairs * 4 * keys * 4 * edge
    return pl.pallas_call(
        functools.partial(centre_kernel, scale, first),
        in_specs=[VMEM] * 6,
        out_specs=[VMEM, VMEM],
        out_shape=[
            pltpu.VMEM((2, cells, pairs * d), BF16),
            pltpu.VMEM((pairs, 2, 2, d + 8, d), F32),
        ],
        cost_estimate=pl.CostEstimate(
            flops=work * 2 * 384, bytes_accessed=4_000_000, transcendentals=work
        ),
        compiler_params=PARAMS,
        name="centre",
    )(pg, up, down, registers, qf, kf)


def edge_kernel(
    scale, parts, p_ref, l_ref, r_ref, cu_ref, cd_ref, qf_ref, kf_ref, *refs
):
    inner, states = refs[:parts], refs[parts : 2 * parts]
    out_ref, edge_ref, sems = refs[2 * parts :]
    _, groups, cells, width = p_ref.shape
    d = LANES
    head = width // HEADS
    edge = RADIUS * RADIUS
    span = cells + edge
    low = lax.broadcasted_iota(jnp.int32, (edge, d), 1) < head
    per = states[0].shape[0]
    copies = []
    for n in range(parts):
        for part in range(2):
            g = 1 if part == 0 else groups - 2
            copies.append(
                (
                    inner[n].at[part],
                    out_ref.at[:, pl.ds(g * RADIUS, RADIUS), pl.ds(n * per * d, per * d)],
                )
            )
    started = copy_all(copies, sems)

    def unit_of(n, i, half, side, exact):
        st = states[n]
        lanes = pl.ds(pl.multiple_of((i + n * per) * d, d), d)
        cells_of = slice(half * edge, (half + 1) * edge)
        halo = l_ref if side == 0 else r_ref
        corner = cu_ref if half == 0 else cd_ref

        def keys(j):
            own = halo[j, :, lanes]
            far = corner[side, j, :, lanes]
            return jnp.concatenate([far, own] if half == 0 else [own, far], axis=0)

        f = kf_ref[side, half * edge : half * edge + span]
        kc = jnp.concatenate([keys(0), f], axis=1)
        g = 0 if side == 0 else groups - 1
        q = p_ref[0, g, cells_of, lanes].astype(F32) * scale
        qf = qf_ref[g, cells_of]
        qc = jnp.concatenate(
            [
                jnp.concatenate([x.astype(BF16), qf], axis=1)
                for x in (jnp.where(low, q, 0.0), jnp.where(low, 0.0, q))
            ],
            axis=0,
        )
        s = dot(kc, qc, NT)
        acc = st[i, half, side, :d]
        high = st[i, half, side, d : d + 1]
        total = st[i, half, side, d + 1 : d + 2]
        if exact:
            new = jnp.maximum(high, jnp.max(s, axis=0, keepdims=True))
            fade = jnp.exp(high - new)
            acc, total, high = acc * fade, total * fade, new
        w = jnp.exp(s - high).astype(BF16)
        total = total + jnp.sum(w.astype(F32), axis=0, keepdims=True)
        yield total
        acc = acc + dot(keys(1), w, TN)
        t = jnp.transpose(acc / total)
        t = jnp.where(low, t[:edge], t[edge:])
        rows_of = slice(half * RADIUS, (half + 1) * RADIUS)
        edge_ref[side, rows_of, :, lanes] = t.reshape(RADIUS, RADIUS, d).astype(BF16)

    for n in range(parts):
        run_guarded(functools.partial(unit_of, n), per, 2 * edge, TOGETHER_E)

    copies = []
    for side in range(2):
        g = 0 if side == 0 else groups - 1
        copies.append(
            (edge_ref.at[side], out_ref.at[:, pl.ds(g * RADIUS, RADIUS)])
        )
    started += copy_all(copies, sems.at[pl.ds(2 * parts, 2)])
    for c in started:
        c.wait()


def edges(pg, left, right, corner_up, corner_down, qf, kf, inner, states, scale, tr, tc):
    _, _, _, width = pg.shape
    parts = len(states)
    return pl.pallas_call(
        functools.partial(edge_kernel, scale, parts),
        in_specs=[VMEM] * (7 + 2 * parts),
        out_specs=HBM,
        out_shape=jax.ShapeDtypeStruct((tr, tc, width), BF16),
        scratch_shapes=[
            pltpu.VMEM((2, tr, RADIUS, width), BF16),
            pltpu.SemaphoreType.DMA((2 * parts + 2,)),
        ],
        cost_estimate=pl.CostEstimate(
            flops=500_000_000, bytes_accessed=3_000_000, transcendentals=800_000
        ),
        compiler_params=PARAMS,
        name="edges",
    )(pg, left, right, corner_up, corner_down, qf, kf, *inner, *states)


def local(patches, registers):
    _, tr, tc, width = patches.shape
    groups = tc // RADIUS
    cells = tr * RADIUS
    edge = RADIUS * RADIUS
    assert tr == 2 * RADIUS and groups == 4 and 2 * width == HEADS * LANES
    scale = (width // HEADS) ** (-0.5)
    row_at, row_n = lax.axis_index("row"), lax.axis_size("row")
    col_at, col_n = lax.axis_index("col"), lax.axis_size("col")

    in_vmem = lambda x: pltpu.with_memory_space_constraint(x, pltpu.VMEM)
    source = pltpu.with_memory_space_constraint(patches, pltpu.HBM)
    left = shift(patches[1:3, :, tc - RADIUS :], "col", 1)
    right = shift(patches[1:3, :, :RADIUS], "col", -1)
    up = shift(patches[1:3, tr - RADIUS :], "row", 1)
    down = shift(patches[1:3, :RADIUS], "row", -1)
    left, right = (x.reshape(2, cells, width) for x in (left, right))
    rows_shape = (2, groups, RADIUS, RADIUS, width)
    up, down = stage(grouped, 2 * groups, up, down, rows_shape)
    up, down = (x.reshape(2, groups, edge, width) for x in (up, down))

    flag = jnp.where((row_at == 0) & (col_at == 0), 0.0, -1e30).astype(F32).reshape(1)
    pg, part = prep(source, registers, flag, scale)
    pg = pg.reshape(3, groups, cells, width)
    part = merge_over(merge_over(part, "row"), "col")
    register_out = (part[0] / part[2]).astype(BF16)

    key_rows = np.repeat(np.arange(-RADIUS, tr + RADIUS), RADIUS)
    key_cols = np.tile(np.arange(RADIUS), tr + 2 * RADIUS)
    stack = lambda cols: np.stack([key_features(key_rows, key_cols + c, tr, tc) for c in cols])
    row = jnp.arange((tr + 2 * RADIUS) * RADIUS, dtype=jnp.int32)[None, :, None]
    off_rows = ((row < edge) & (row_at == 0)) | ((row >= edge + cells) & (row_at == row_n - 1))
    side = jnp.arange(2, dtype=jnp.int32)[:, None, None]
    off_cols = ((side == 0) & (col_at == 0)) | ((side == 1) & (col_at == col_n - 1))
    off_lane = LANES - 1
    kf = with_grid_edge(stack([g * RADIUS for g in range(groups)]), (off_rows, off_lane))
    kf_side = with_grid_edge(stack([-RADIUS, tc]), (off_rows | off_cols, off_lane))
    q_rows = np.repeat(np.arange(tr), RADIUS)
    q_cols = np.tile(np.arange(RADIUS), tr)
    qf = np.stack([query_features(q_rows, q_cols + g * RADIUS, tr, tc) for g in range(groups)])
    qf[..., off_lane] = 1.0
    qf = jnp.asarray(qf.astype(BF16))

    pairs = HEADS // 2
    parts = PARTS
    per = pairs // parts
    done = []
    for n in range(parts):
        done.append(centre(pg, up, down, registers, qf, kf, scale, n * per, per))
    near_l, near_r, first_state = lax.optimization_barrier((left, right, done[0][1]))
    done[0] = (done[0][0], first_state)
    bottom = jnp.stack([near_l[:, -edge:], near_r[:, -edge:]])
    corner_up = in_vmem(shift(bottom, "row", 1))
    top = jnp.stack([near_l[:, :edge], near_r[:, :edge]])
    corner_down = in_vmem(shift(top, "row", -1))
    left, right = stage(whole, 2, near_l, near_r, left.shape)
    inner = [x[0].reshape(2, tr, RADIUS, per * LANES) for x in done]
    out = edges(
        pg, left, right, corner_up, corner_down, qf, kf_side, inner, [x[1] for x in done], scale, tr, tc
    )
    return (out, register_out)


def solution(mesh):
    in_specs = (P(None, "row", "col", None), P())
    out_specs = (P("row", "col", None), P())
    return jax.shard_map(local, mesh=mesh, in_specs=in_specs, out_specs=out_specs, check_vma=False)
```

```python
import functools

import jax
import jax.numpy as jnp
import numpy as np
from jax import lax
from jax.experimental import pallas as pl
from jax.experimental.pallas import tpu as pltpu
from jax.sharding import PartitionSpec as P


HEADS = 16
PARTS = 1
TOGETHER_C = 2
TOGETHER_E = 2
RADIUS = 8
FAR = -30000.0
LEAST, MOST = 1e-20, 1e30
LANES = 128
F32 = jnp.float32
BF16 = jnp.bfloat16
NT = (((1,), (1,)), ((), ()))
NN = (((1,), (0,)), ((), ()))
TN = (((0,), (0,)), ((), ()))
VMEM = pl.BlockSpec(memory_space=pltpu.VMEM)
HBM = pl.BlockSpec(memory_space=pltpu.HBM)
SMEM = pl.BlockSpec(memory_space=pltpu.SMEM)
PARAMS = pltpu.CompilerParams(vmem_limit_bytes=24 * 1024 * 1024)


def dot(a, b, dims):
    return lax.dot_general(a, b, dims, preferred_element_type=F32)


def shift(x, axis, step):
    n = lax.axis_size(axis)
    return lax.ppermute(x, axis, [(i, i + step) for i in range(n) if 0 <= i + step < n])


def key_features(rows, cols, tr, tc):
    lane = np.arange(LANES)
    far_col = (lane < tc) & (np.abs(cols[..., None] - lane) > RADIUS)
    far_row = (lane >= tc) & (lane < tc + tr) & (np.abs(rows[..., None] - (lane - tc)) > RADIUS)
    return np.where(far_col | far_row, FAR, 0.0).astype(np.float32)


def query_features(rows, cols, tr, tc):
    lane = np.arange(LANES)
    hit = (lane == cols[..., None]) | (lane - tc == rows[..., None]) | (lane == tc + tr)
    return hit.astype(np.float32)


def with_grid_edge(const, off):
    lane = lax.broadcasted_iota(jnp.int32, const.shape, const.ndim - 1)
    return jnp.where((lane == off[1]) & off[0], FAR, jnp.asarray(const)).astype(BF16)


def copy_all(copies, sems):
    started = []
    for i, (src, dst) in enumerate(copies):
        c = pltpu.make_async_copy(src, dst, sems.at[i])
        c.start()
        started.append(c)
    return started


def stage_kernel(copies_of, a_ref, b_ref, a_out, b_out, sems):
    copies = copies_of(a_ref, a_out) + copies_of(b_ref, b_out)
    for c in copy_all(copies, sems):
        c.wait()


def whole(src, dst):
    return [(src.at[j], dst.at[j]) for j in range(2)]


def stage(copies_of, count, a, b, shape):
    a, b = (pltpu.with_memory_space_constraint(x, pltpu.HBM) for x in (a, b))
    return pl.pallas_call(
        functools.partial(stage_kernel, copies_of),
        in_specs=[HBM, HBM],
        out_specs=[VMEM, VMEM],
        out_shape=[pltpu.VMEM(shape, BF16)] * 2,
        scratch_shapes=[pltpu.SemaphoreType.DMA((2 * count,))],
        cost_estimate=pl.CostEstimate(flops=1_000_000, bytes_accessed=4_000_000, transcendentals=0),
        compiler_params=PARAMS,
    )(a, b)


def load_kernel(p_ref, out_ref, right_ref, left_ref, down_ref, up_ref, load_sems, send_sems):
    groups = out_ref.shape[1]
    tr = out_ref.shape[2]
    order = (0, groups - 1) + tuple(range(1, groups - 1))
    loads = {}
    for g in order:
        for j in (1, 2):
            loads[j, g] = (p_ref.at[j, :, pl.ds(g * RADIUS, RADIUS)], out_ref.at[j, g])
    for g in order:
        loads[0, g] = (p_ref.at[0, :, pl.ds(g * RADIUS, RADIUS)], out_ref.at[0, g])
    started = dict(zip(loads, copy_all(loads.values(), load_sems)))
    sends = []
    for g, ref in ((groups - 1, right_ref), (0, left_ref)):
        for j in (1, 2):
            started[j, g].wait()
            c = pltpu.make_async_copy(out_ref.at[j, g], ref.at[j - 1], send_sems.at[len(sends)])
            c.start()
            sends.append(c)
    for g in order[2:]:
        for j in (1, 2):
            started[j, g].wait()
    for ref, rows in ((down_ref, pl.ds(tr - RADIUS, RADIUS)), (up_ref, pl.ds(0, RADIUS))):
        for j in (1, 2):
            c = pltpu.make_async_copy(
                out_ref.at[j, :, rows], ref.at[j - 1], send_sems.at[len(sends)]
            )
            c.start()
            sends.append(c)
    for g in order:
        started[0, g].wait()
    for c in sends:
        c.wait()


def load(patches):
    _, tr, tc, width = patches.shape
    groups = tc // RADIUS
    side = jax.ShapeDtypeStruct((2, tr, RADIUS, width), BF16)
    rows = jax.ShapeDtypeStruct((2, groups, RADIUS, RADIUS, width), BF16)
    return pl.pallas_call(
        load_kernel,
        in_specs=[HBM],
        out_specs=[VMEM] + [HBM] * 4,
        out_shape=[pltpu.VMEM((3, groups, tr, RADIUS, width), BF16), side, side, rows, rows],
        scratch_shapes=[pltpu.SemaphoreType.DMA((3 * groups,)), pltpu.SemaphoreType.DMA((8,))],
        compiler_params=PARAMS,
        name="load",
    )(pltpu.with_memory_space_constraint(patches, pltpu.HBM))


def prep_kernel(scale, flag_ref, reg_ref, p_ref, part_ref):
    width = p_ref.shape[-1]
    count = reg_ref.shape[1]
    head = width // HEADS
    lane_head = lax.broadcasted_iota(jnp.int32, (HEADS, count, width), 2) // head
    own = lane_head == lax.broadcasted_iota(jnp.int32, (HEADS, count, width), 0)
    q = reg_ref[0].astype(F32) * scale
    q = jnp.where(own, q[None], 0.0).reshape(HEADS * count, width).astype(BF16)
    self_scores = dot(reg_ref[1], q, NT) + flag_ref[0]
    scores = dot(p_ref[1].reshape(-1, width), q, NT)
    high = jnp.maximum(
        jnp.max(scores, axis=0, keepdims=True), jnp.max(self_scores, axis=0, keepdims=True)
    )
    w = jnp.exp(scores - high)
    self_w = jnp.exp(self_scores - high)
    total = jnp.sum(w, axis=0, keepdims=True) + jnp.sum(self_w, axis=0, keepdims=True)
    wt = jnp.transpose(w).astype(BF16)
    acc = dot(wt, p_ref[2].reshape(-1, width), NN)
    acc = acc + dot(jnp.transpose(self_w).astype(BF16), reg_ref[2], NN)
    acc = jnp.sum(jnp.where(own, acc.reshape(HEADS, count, width), 0.0), axis=0)
    n = HEADS * count

    def spread(row):
        col = jnp.transpose(jnp.broadcast_to(row, (LANES, n))).reshape(HEADS, count, LANES)
        low = lax.broadcasted_iota(jnp.int32, (count, LANES), 1) < head
        return jnp.concatenate(
            [jnp.where(low, col[2 * p], col[2 * p + 1]) for p in range(HEADS // 2)], axis=1
        )

    part_ref[0] = acc
    part_ref[1] = spread(high)
    part_ref[2] = spread(total)


def prep(pg, registers, flag, scale):
    width = pg.shape[-1]
    count = registers.shape[1]
    return pl.pallas_call(
        functools.partial(prep_kernel, scale),
        in_specs=[SMEM, VMEM, VMEM],
        out_specs=VMEM,
        out_shape=pltpu.VMEM((3, count, width), F32),
        cost_estimate=pl.CostEstimate(
            flops=300_000_000, bytes_accessed=2_000_000, transcendentals=70_000
        ),
        compiler_params=PARAMS,
        name="prep",
    )(flag, registers, pg)


def merge(a, b):
    high = jnp.maximum(a[1], b[1])
    fa = jnp.exp(a[1] - high)
    fb = jnp.exp(b[1] - high)
    return jnp.stack([a[0] * fa + b[0] * fb, high, a[2] * fa + b[2] * fb])


def merge_all(part, late):
    for axis in ("row", "col"):
        n = lax.axis_size(axis)
        if n & (n - 1):
            every = lax.all_gather(part, axis)
            part = functools.reduce(merge, [every[i] for i in range(n)])
            continue
        step = 1
        while step < n:
            other = lax.ppermute(part, axis, [(i, i ^ step) for i in range(n)])
            if axis == "row" and 2 * step == n:
                other, late = lax.optimization_barrier((other, late))
            part = merge(part, other)
            step *= 2
    return part, late


def centre_kernel(scale, first, p_ref, up_ref, down_ref, reg_ref, qf_ref, kf_ref, in_ref, st_ref):
    _, groups, cells, width = p_ref.shape
    d = LANES
    head = width // HEADS
    edge = RADIUS * RADIUS
    low = lax.broadcasted_iota(jnp.int32, (edge, d), 1) < head
    pad = lax.broadcasted_iota(jnp.int32, (2 * RADIUS, d), 0) >= RADIUS
    off = lax.broadcasted_iota(jnp.int32, (2 * RADIUS, d), 1) == d - 1
    reg_f = jnp.where(pad & off, FAR, 0.0).astype(BF16)
    zero = jnp.zeros((RADIUS, d), BF16)

    def unit(i, half, part, exact):
        lanes = pl.ds(pl.multiple_of((i + first) * d, d), d)
        lanes_out = pl.ds(pl.multiple_of(i * d, d), d)
        rows = slice(half * edge, (half + 1) * edge)
        near = range(part, part + 3)
        span = cells + edge

        def stacked(j):
            pieces = []
            for g in near:
                own = p_ref[j, g, :, lanes]
                if half == 0:
                    pieces += [up_ref[j - 1, g, :, lanes], own]
                else:
                    pieces += [own, down_ref[j - 1, g, :, lanes]]
            return jnp.concatenate(pieces + [reg_ref[j, :, lanes], zero], axis=0)

        f = jnp.concatenate(
            [kf_ref[g, half * edge : half * edge + span] for g in near] + [reg_f], axis=0
        )
        kc = jnp.concatenate([stacked(1), f], axis=1)
        qs = []
        for g in (0, 1) if part == 0 else (groups - 1, groups - 2):
            q = p_ref[0, g, rows, lanes].astype(F32) * scale
            qf = qf_ref[g, rows]
            for x in (jnp.where(low, q, 0.0), jnp.where(low, 0.0, q)):
                qs.append(jnp.concatenate([x.astype(BF16), qf], axis=1))
        s = dot(kc, jnp.concatenate(qs, axis=0), NT)
        if exact:
            high = jnp.max(s, axis=0, keepdims=True)
            s = s - high
        else:
            high = jnp.zeros((1, s.shape[1]), F32)
        w = jnp.exp(s).astype(BF16)
        total = jnp.sum(w.astype(F32), axis=0, keepdims=True)
        yield total
        o = dot(stacked(2), w, TN)
        st_ref[i, half, part, :d] = o[:, :d]
        st_ref[i, half, part, d : d + 8] = jnp.concatenate(
            [high[:, :d], total[:, :d], jnp.zeros((6, d), F32)], axis=0
        )
        t = jnp.transpose(o[:, d:] / total[:, d:])
        t = jnp.where(low, t[:edge], t[edge:])
        in_ref[part, rows, lanes_out] = t.astype(BF16)

    run_guarded(unit, st_ref.shape[0], 4 * edge, TOGETHER_C)


def run_guarded(unit, count, lanes, together=1):
    units = [(half, part) for half in range(2) for part in range(2)]

    def both(i, exact):
        step = 1 if exact else together
        running = [
            unit(i * step + k, half, part, exact) for k in range(step) for half, part in units
        ]
        totals = [next(r) for r in running]
        for r in running:
            next(r, None)
        return totals

    def fast(i, seen):
        least, most = seen
        for total in both(i, False):
            least = jnp.where(total >= least, least, total)
            most = jnp.where(total <= most, most, total)
        return least, most

    one = jnp.ones((1, lanes), F32)
    least, most = lax.fori_loop(0, count // together, fast, (one, one))
    fine = jnp.where((least > LEAST) & (most < MOST), 1.0, 0.0)

    @pl.when(jnp.min(fine) < 0.5)
    def _():
        @pl.loop(0, count)
        def _(i):
            both(i, True)


def centre(pg, up, down, registers, qf, kf, scale, first, pairs):
    _, _, cells, _ = pg.shape
    edge = RADIUS * RADIUS
    d = LANES
    keys = 3 * (cells + edge) + 2 * RADIUS
    work = pairs * 4 * keys * 4 * edge
    return pl.pallas_call(
        functools.partial(centre_kernel, scale, first),
        in_specs=[VMEM] * 6,
        out_specs=[VMEM, VMEM],
        out_shape=[
            pltpu.VMEM((2, cells, pairs * d), BF16),
            pltpu.VMEM((pairs, 2, 2, d + 8, d), F32),
        ],
        cost_estimate=pl.CostEstimate(
            flops=work * 2 * 384, bytes_accessed=4_000_000, transcendentals=work
        ),
        compiler_params=PARAMS,
        name="centre",
    )(pg, up, down, registers, qf, kf)


def edge_kernel(
    scale, parts, p_ref, l_ref, r_ref, cu_ref, cd_ref, qf_ref, kf_ref, *refs
):
    inner, states = refs[:parts], refs[parts : 2 * parts]
    out_ref, edge_ref, sems = refs[2 * parts :]
    _, groups, cells, width = p_ref.shape
    d = LANES
    head = width // HEADS
    edge = RADIUS * RADIUS
    span = cells + edge
    low = lax.broadcasted_iota(jnp.int32, (edge, d), 1) < head
    per = states[0].shape[0]
    copies = []
    for n in range(parts):
        for part in range(2):
            g = 1 if part == 0 else groups - 2
            copies.append(
                (
                    inner[n].at[part],
                    out_ref.at[:, pl.ds(g * RADIUS, RADIUS), pl.ds(n * per * d, per * d)],
                )
            )
    started = copy_all(copies, sems)

    def unit_of(n, i, half, side, exact):
        st = states[n]
        lanes = pl.ds(pl.multiple_of((i + n * per) * d, d), d)
        cells_of = slice(half * edge, (half + 1) * edge)
        halo = l_ref if side == 0 else r_ref
        corner = cu_ref if half == 0 else cd_ref

        def keys(j):
            own = halo[j, :, lanes]
            far = corner[side, j, :, lanes]
            return jnp.concatenate([far, own] if half == 0 else [own, far], axis=0)

        f = kf_ref[side, half * edge : half * edge + span]
        kc = jnp.concatenate([keys(0), f], axis=1)
        g = 0 if side == 0 else groups - 1
        q = p_ref[0, g, cells_of, lanes].astype(F32) * scale
        qf = qf_ref[g, cells_of]
        qc = jnp.concatenate(
            [
                jnp.concatenate([x.astype(BF16), qf], axis=1)
                for x in (jnp.where(low, q, 0.0), jnp.where(low, 0.0, q))
            ],
            axis=0,
        )
        s = dot(kc, qc, NT)
        acc = st[i, half, side, :d]
        high = st[i, half, side, d : d + 1]
        total = st[i, half, side, d + 1 : d + 2]
        if exact:
            new = jnp.maximum(high, jnp.max(s, axis=0, keepdims=True))
            fade = jnp.exp(high - new)
            acc, total, high = acc * fade, total * fade, new
        w = jnp.exp(s - high).astype(BF16)
        total = total + jnp.sum(w.astype(F32), axis=0, keepdims=True)
        yield total
        acc = acc + dot(keys(1), w, TN)
        t = jnp.transpose(acc / total)
        t = jnp.where(low, t[:edge], t[edge:])
        rows_of = slice(half * RADIUS, (half + 1) * RADIUS)
        edge_ref[side, rows_of, :, lanes] = t.reshape(RADIUS, RADIUS, d).astype(BF16)

    for n in range(parts):
        run_guarded(functools.partial(unit_of, n), per, 2 * edge, TOGETHER_E)

    copies = []
    for side in range(2):
        g = 0 if side == 0 else groups - 1
        copies.append(
            (edge_ref.at[side], out_ref.at[:, pl.ds(g * RADIUS, RADIUS)])
        )
    started += copy_all(copies, sems.at[pl.ds(2 * parts, 2)])
    for c in started:
        c.wait()


def edges(pg, left, right, corner_up, corner_down, qf, kf, inner, states, scale, tr, tc):
    _, _, _, width = pg.shape
    parts = len(states)
    return pl.pallas_call(
        functools.partial(edge_kernel, scale, parts),
        in_specs=[VMEM] * (7 + 2 * parts),
        out_specs=HBM,
        out_shape=jax.ShapeDtypeStruct((tr, tc, width), BF16),
        scratch_shapes=[
            pltpu.VMEM((2, tr, RADIUS, width), BF16),
            pltpu.SemaphoreType.DMA((2 * parts + 2,)),
        ],
        cost_estimate=pl.CostEstimate(
            flops=500_000_000, bytes_accessed=3_000_000, transcendentals=800_000
        ),
        compiler_params=PARAMS,
        name="edges",
    )(pg, left, right, corner_up, corner_down, qf, kf, *inner, *states)


def local(patches, registers):
    _, tr, tc, width = patches.shape
    groups = tc // RADIUS
    cells = tr * RADIUS
    edge = RADIUS * RADIUS
    assert tr == 2 * RADIUS and groups == 4 and 2 * width == HEADS * LANES
    scale = (width // HEADS) ** (-0.5)
    row_at, row_n = lax.axis_index("row"), lax.axis_size("row")
    col_at, col_n = lax.axis_index("col"), lax.axis_size("col")

    in_vmem = lambda x: pltpu.with_memory_space_constraint(x, pltpu.VMEM)
    pg, to_right, to_left, to_down, to_up = load(patches)
    left = shift(to_right, "col", 1)
    right = shift(to_left, "col", -1)
    up = shift(to_down, "row", 1)
    down = shift(to_up, "row", -1)
    left, right = (x.reshape(2, cells, width) for x in (left, right))
    rows_shape = (2, groups, RADIUS, RADIUS, width)
    up, down = stage(whole, 2, up, down, rows_shape)
    up, down = (x.reshape(2, groups, edge, width) for x in (up, down))

    flag = jnp.where((row_at == 0) & (col_at == 0), 0.0, -1e30).astype(F32).reshape(1)
    pg = pg.reshape(3, groups, cells, width)
    part = prep(pg, registers, flag, scale)

    key_rows = np.repeat(np.arange(-RADIUS, tr + RADIUS), RADIUS)
    key_cols = np.tile(np.arange(RADIUS), tr + 2 * RADIUS)
    stack = lambda cols: np.stack([key_features(key_rows, key_cols + c, tr, tc) for c in cols])
    row = jnp.arange((tr + 2 * RADIUS) * RADIUS, dtype=jnp.int32)[None, :, None]
    off_rows = ((row < edge) & (row_at == 0)) | ((row >= edge + cells) & (row_at == row_n - 1))
    side = jnp.arange(2, dtype=jnp.int32)[:, None, None]
    off_cols = ((side == 0) & (col_at == 0)) | ((side == 1) & (col_at == col_n - 1))
    off_lane = LANES - 1
    kf = with_grid_edge(stack([g * RADIUS for g in range(groups)]), (off_rows, off_lane))
    kf_side = with_grid_edge(stack([-RADIUS, tc]), (off_rows | off_cols, off_lane))
    q_rows = np.repeat(np.arange(tr), RADIUS)
    q_cols = np.tile(np.arange(RADIUS), tr)
    qf = np.stack([query_features(q_rows, q_cols + g * RADIUS, tr, tc) for g in range(groups)])
    qf[..., off_lane] = 1.0
    qf = jnp.asarray(qf.astype(BF16))

    pairs = HEADS // 2
    parts = PARTS
    per = pairs // parts
    done = []
    for n in range(parts):
        done.append(centre(pg, up, down, registers, qf, kf, scale, n * per, per))
    near_l, near_r, first_state = lax.optimization_barrier((left, right, done[0][1]))
    done[0] = (done[0][0], first_state)
    bottom = jnp.stack([near_l[:, -edge:], near_r[:, -edge:]])
    corner_up = in_vmem(shift(bottom, "row", 1))
    top = jnp.stack([near_l[:, :edge], near_r[:, :edge]])
    corner_down = in_vmem(shift(top, "row", -1))
    part, first_state = merge_all(part, done[0][1])
    done[0] = (done[0][0], first_state)
    register_out = (part[0] / part[2]).astype(BF16)
    left, right = stage(whole, 2, near_l, near_r, left.shape)
    inner = [x[0].reshape(2, tr, RADIUS, per * LANES) for x in done]
    states = [x[1] for x in done]
    out = edges(pg, left, right, corner_up, corner_down, qf, kf_side, inner, states, scale, tr, tc)
    return (out, register_out)


def solution(mesh):
    in_specs = (P(None, "row", "col", None), P())
    out_specs = (P("row", "col", None), P())
    return jax.shard_map(local, mesh=mesh, in_specs=in_specs, out_specs=out_specs, check_vma=False)
```

```python
import functools

import jax
import jax.numpy as jnp
import numpy as np
from jax import lax
from jax.experimental import pallas as pl
from jax.experimental.pallas import tpu as pltpu
from jax.sharding import PartitionSpec as P


HEADS = 16
PARTS = 1
TOGETHER_C = 2
TOGETHER_E = 4
RADIUS = 8
FAR = -30000.0
LEAST, MOST = 1e-20, 1e30
LANES = 128
F32 = jnp.float32
BF16 = jnp.bfloat16
NT = (((1,), (1,)), ((), ()))
NN = (((1,), (0,)), ((), ()))
TN = (((0,), (0,)), ((), ()))
VMEM = pl.BlockSpec(memory_space=pltpu.VMEM)
HBM = pl.BlockSpec(memory_space=pltpu.HBM)
SMEM = pl.BlockSpec(memory_space=pltpu.SMEM)
PARAMS = pltpu.CompilerParams(vmem_limit_bytes=24 * 1024 * 1024)


def dot(a, b, dims):
    return lax.dot_general(a, b, dims, preferred_element_type=F32)


def shift(x, axis, step):
    n = lax.axis_size(axis)
    return lax.ppermute(x, axis, [(i, i + step) for i in range(n) if 0 <= i + step < n])


def key_features(rows, cols, tr, tc):
    lane = np.arange(LANES)
    far_col = (lane < tc) & (np.abs(cols[..., None] - lane) > RADIUS)
    far_row = (lane >= tc) & (lane < tc + tr) & (np.abs(rows[..., None] - (lane - tc)) > RADIUS)
    return np.where(far_col | far_row, FAR, 0.0).astype(np.float32)


def query_features(rows, cols, tr, tc):
    lane = np.arange(LANES)
    hit = (lane == cols[..., None]) | (lane - tc == rows[..., None]) | (lane == tc + tr)
    return hit.astype(np.float32)


def with_grid_edge(const, off):
    lane = lax.broadcasted_iota(jnp.int32, const.shape, const.ndim - 1)
    return jnp.where((lane == off[1]) & off[0], FAR, jnp.asarray(const)).astype(BF16)


def copy_all(copies, sems):
    started = []
    for i, (src, dst) in enumerate(copies):
        c = pltpu.make_async_copy(src, dst, sems.at[i])
        c.start()
        started.append(c)
    return started


def stage_kernel(copies_of, a_ref, b_ref, a_out, b_out, sems):
    copies = copies_of(a_ref, a_out) + copies_of(b_ref, b_out)
    for c in copy_all(copies, sems):
        c.wait()


def whole(src, dst):
    return [(src.at[j], dst.at[j]) for j in range(2)]


def stage(copies_of, count, a, b, shape):
    a, b = (pltpu.with_memory_space_constraint(x, pltpu.HBM) for x in (a, b))
    return pl.pallas_call(
        functools.partial(stage_kernel, copies_of),
        in_specs=[HBM, HBM],
        out_specs=[VMEM, VMEM],
        out_shape=[pltpu.VMEM(shape, BF16)] * 2,
        scratch_shapes=[pltpu.SemaphoreType.DMA((2 * count,))],
        cost_estimate=pl.CostEstimate(flops=1_000_000, bytes_accessed=4_000_000, transcendentals=0),
        compiler_params=PARAMS,
    )(a, b)


def load_kernel(p_ref, out_ref, right_ref, left_ref, down_ref, up_ref, load_sems, send_sems):
    groups = out_ref.shape[1]
    tr = out_ref.shape[2]
    order = (0, groups - 1) + tuple(range(1, groups - 1))
    loads = {}
    for g in order:
        for j in (1, 2):
            loads[j, g] = (p_ref.at[j, :, pl.ds(g * RADIUS, RADIUS)], out_ref.at[j, g])
    for g in order:
        loads[0, g] = (p_ref.at[0, :, pl.ds(g * RADIUS, RADIUS)], out_ref.at[0, g])
    started = dict(zip(loads, copy_all(loads.values(), load_sems)))
    sends = []
    for g, ref in ((groups - 1, right_ref), (0, left_ref)):
        for j in (1, 2):
            started[j, g].wait()
            c = pltpu.make_async_copy(out_ref.at[j, g], ref.at[j - 1], send_sems.at[len(sends)])
            c.start()
            sends.append(c)
    for g in order[2:]:
        for j in (1, 2):
            started[j, g].wait()
    for ref, rows in ((down_ref, pl.ds(tr - RADIUS, RADIUS)), (up_ref, pl.ds(0, RADIUS))):
        for j in (1, 2):
            c = pltpu.make_async_copy(
                out_ref.at[j, :, rows], ref.at[j - 1], send_sems.at[len(sends)]
            )
            c.start()
            sends.append(c)
    for g in order:
        started[0, g].wait()
    for c in sends:
        c.wait()


def load(patches):
    _, tr, tc, width = patches.shape
    groups = tc // RADIUS
    side = jax.ShapeDtypeStruct((2, tr, RADIUS, width), BF16)
    rows = jax.ShapeDtypeStruct((2, groups, RADIUS, RADIUS, width), BF16)
    return pl.pallas_call(
        load_kernel,
        in_specs=[HBM],
        out_specs=[VMEM] + [HBM] * 4,
        out_shape=[pltpu.VMEM((3, groups, tr, RADIUS, width), BF16), side, side, rows, rows],
        scratch_shapes=[pltpu.SemaphoreType.DMA((3 * groups,)), pltpu.SemaphoreType.DMA((8,))],
        compiler_params=PARAMS,
        name="load",
    )(pltpu.with_memory_space_constraint(patches, pltpu.HBM))


def prep_kernel(scale, flag_ref, reg_ref, p_ref, part_ref):
    width = p_ref.shape[-1]
    count = reg_ref.shape[1]
    head = width // HEADS
    lane_head = lax.broadcasted_iota(jnp.int32, (HEADS, count, width), 2) // head
    own = lane_head == lax.broadcasted_iota(jnp.int32, (HEADS, count, width), 0)
    q = reg_ref[0].astype(F32) * scale
    q = jnp.where(own, q[None], 0.0).reshape(HEADS * count, width).astype(BF16)
    self_scores = dot(reg_ref[1], q, NT) + flag_ref[0]
    scores = dot(p_ref[1].reshape(-1, width), q, NT)
    high = jnp.maximum(
        jnp.max(scores, axis=0, keepdims=True), jnp.max(self_scores, axis=0, keepdims=True)
    )
    w = jnp.exp(scores - high)
    self_w = jnp.exp(self_scores - high)
    total = jnp.sum(w, axis=0, keepdims=True) + jnp.sum(self_w, axis=0, keepdims=True)
    wt = jnp.transpose(w).astype(BF16)
    acc = dot(wt, p_ref[2].reshape(-1, width), NN)
    acc = acc + dot(jnp.transpose(self_w).astype(BF16), reg_ref[2], NN)
    acc = jnp.sum(jnp.where(own, acc.reshape(HEADS, count, width), 0.0), axis=0)
    n = HEADS * count

    def spread(row):
        col = jnp.transpose(jnp.broadcast_to(row, (LANES, n))).reshape(HEADS, count, LANES)
        low = lax.broadcasted_iota(jnp.int32, (count, LANES), 1) < head
        return jnp.concatenate(
            [jnp.where(low, col[2 * p], col[2 * p + 1]) for p in range(HEADS // 2)], axis=1
        )

    part_ref[0] = acc
    part_ref[1] = spread(high)
    part_ref[2] = spread(total)


def prep(pg, registers, flag, scale):
    width = pg.shape[-1]
    count = registers.shape[1]
    return pl.pallas_call(
        functools.partial(prep_kernel, scale),
        in_specs=[SMEM, VMEM, VMEM],
        out_specs=VMEM,
        out_shape=pltpu.VMEM((3, count, width), F32),
        cost_estimate=pl.CostEstimate(
            flops=300_000_000, bytes_accessed=2_000_000, transcendentals=70_000
        ),
        compiler_params=PARAMS,
        name="prep",
    )(flag, registers, pg)


def merge(a, b):
    high = jnp.maximum(a[1], b[1])
    fa = jnp.exp(a[1] - high)
    fb = jnp.exp(b[1] - high)
    return jnp.stack([a[0] * fa + b[0] * fb, high, a[2] * fa + b[2] * fb])


def merge_over(part, axis, late=None):
    n = lax.axis_size(axis)
    if n & (n - 1):
        every = lax.all_gather(part, axis)
        return functools.reduce(merge, [every[i] for i in range(n)]), late
    step = 1
    while step < n:
        other = lax.ppermute(part, axis, [(i, i ^ step) for i in range(n)])
        if step == 2 and late is not None:
            other, late = lax.optimization_barrier((other, late))
        part = merge(part, other)
        step *= 2
    return part, late


def centre_kernel(scale, first, p_ref, up_ref, down_ref, reg_ref, qf_ref, kf_ref, in_ref, st_ref):
    _, groups, cells, width = p_ref.shape
    d = LANES
    head = width // HEADS
    edge = RADIUS * RADIUS
    low = lax.broadcasted_iota(jnp.int32, (edge, d), 1) < head
    pad = lax.broadcasted_iota(jnp.int32, (2 * RADIUS, d), 0) >= RADIUS
    off = lax.broadcasted_iota(jnp.int32, (2 * RADIUS, d), 1) == d - 1
    reg_f = jnp.where(pad & off, FAR, 0.0).astype(BF16)
    zero = jnp.zeros((RADIUS, d), BF16)

    def unit(i, half, part, exact):
        lanes = pl.ds(pl.multiple_of((i + first) * d, d), d)
        lanes_out = pl.ds(pl.multiple_of(i * d, d), d)
        rows = slice(half * edge, (half + 1) * edge)
        near = range(part, part + 3)
        span = cells + edge

        def stacked(j):
            pieces = []
            for g in near:
                own = p_ref[j, g, :, lanes]
                if half == 0:
                    pieces += [up_ref[j - 1, g, :, lanes], own]
                else:
                    pieces += [own, down_ref[j - 1, g, :, lanes]]
            return jnp.concatenate(pieces + [reg_ref[j, :, lanes], zero], axis=0)

        f = jnp.concatenate(
            [kf_ref[g, half * edge : half * edge + span] for g in near] + [reg_f], axis=0
        )
        kc = jnp.concatenate([stacked(1), f], axis=1)
        qs = []
        for g in (0, 1) if part == 0 else (groups - 1, groups - 2):
            q = p_ref[0, g, rows, lanes].astype(F32) * scale
            qf = qf_ref[g, rows]
            for x in (jnp.where(low, q, 0.0), jnp.where(low, 0.0, q)):
                qs.append(jnp.concatenate([x.astype(BF16), qf], axis=1))
        s = dot(kc, jnp.concatenate(qs, axis=0), NT)
        if exact:
            high = jnp.max(s, axis=0, keepdims=True)
            s = s - high
        else:
            high = jnp.zeros((1, s.shape[1]), F32)
        w = jnp.exp(s).astype(BF16)
        total = jnp.sum(w.astype(F32), axis=0, keepdims=True)
        yield total
        o = dot(stacked(2), w, TN)
        st_ref[i, half, part, :d] = o[:, :d]
        st_ref[i, half, part, d : d + 8] = jnp.concatenate(
            [high[:, :d], total[:, :d], jnp.zeros((6, d), F32)], axis=0
        )
        t = jnp.transpose(o[:, d:] / total[:, d:])
        t = jnp.where(low, t[:edge], t[edge:])
        in_ref[part, rows, lanes_out] = t.astype(BF16)

    run_guarded(unit, st_ref.shape[0], 4 * edge, TOGETHER_C)


def run_guarded(unit, count, lanes, together=1):
    units = [(half, part) for half in range(2) for part in range(2)]

    def both(i, exact):
        step = 1 if exact else together
        running = [
            unit(i * step + k, half, part, exact) for k in range(step) for half, part in units
        ]
        totals = [next(r) for r in running]
        for r in running:
            next(r, None)
        return totals

    def fast(i, seen):
        least, most = seen
        for total in both(i, False):
            least = jnp.where(total >= least, least, total)
            most = jnp.where(total <= most, most, total)
        return least, most

    one = jnp.ones((1, lanes), F32)
    least, most = lax.fori_loop(0, count // together, fast, (one, one))
    fine = jnp.where((least > LEAST) & (most < MOST), 1.0, 0.0)

    @pl.when(jnp.min(fine) < 0.5)
    def _():
        @pl.loop(0, count)
        def _(i):
            both(i, True)


def centre(pg, up, down, registers, qf, kf, scale, first, pairs):
    _, _, cells, _ = pg.shape
    edge = RADIUS * RADIUS
    d = LANES
    keys = 3 * (cells + edge) + 2 * RADIUS
    work = pairs * 4 * keys * 4 * edge
    return pl.pallas_call(
        functools.partial(centre_kernel, scale, first),
        in_specs=[VMEM] * 6,
        out_specs=[VMEM, VMEM],
        out_shape=[
            pltpu.VMEM((2, cells, pairs * d), BF16),
            pltpu.VMEM((pairs, 2, 2, d + 8, d), F32),
        ],
        cost_estimate=pl.CostEstimate(
            flops=work * 2 * 384, bytes_accessed=4_000_000, transcendentals=work
        ),
        compiler_params=PARAMS,
        name="centre",
    )(pg, up, down, registers, qf, kf)


def edge_kernel(
    scale, parts, p_ref, l_ref, r_ref, cu_ref, cd_ref, qf_ref, kf_ref, *refs
):
    inner, states = refs[:parts], refs[parts : 2 * parts]
    out_ref, edge_ref, sems = refs[2 * parts :]
    _, groups, cells, width = p_ref.shape
    d = LANES
    head = width // HEADS
    edge = RADIUS * RADIUS
    span = cells + edge
    low = lax.broadcasted_iota(jnp.int32, (edge, d), 1) < head
    per = states[0].shape[0]
    copies = []
    for n in range(parts):
        for part in range(2):
            g = 1 if part == 0 else groups - 2
            copies.append(
                (
                    inner[n].at[part],
                    out_ref.at[:, pl.ds(g * RADIUS, RADIUS), pl.ds(n * per * d, per * d)],
                )
            )
    started = copy_all(copies, sems)

    def unit_of(n, i, half, side, exact):
        st = states[n]
        lanes = pl.ds(pl.multiple_of((i + n * per) * d, d), d)
        cells_of = slice(half * edge, (half + 1) * edge)
        halo = l_ref if side == 0 else r_ref
        corner = cu_ref if half == 0 else cd_ref

        def keys(j):
            own = halo[j, :, lanes]
            far = corner[side, j, :, lanes]
            return jnp.concatenate([far, own] if half == 0 else [own, far], axis=0)

        f = kf_ref[side, half * edge : half * edge + span]
        kc = jnp.concatenate([keys(0), f], axis=1)
        g = 0 if side == 0 else groups - 1
        q = p_ref[0, g, cells_of, lanes].astype(F32) * scale
        qf = qf_ref[g, cells_of]
        qc = jnp.concatenate(
            [
                jnp.concatenate([x.astype(BF16), qf], axis=1)
                for x in (jnp.where(low, q, 0.0), jnp.where(low, 0.0, q))
            ],
            axis=0,
        )
        s = dot(kc, qc, NT)
        acc = st[i, half, side, :d]
        high = st[i, half, side, d : d + 1]
        total = st[i, half, side, d + 1 : d + 2]
        if exact:
            new = jnp.maximum(high, jnp.max(s, axis=0, keepdims=True))
            fade = jnp.exp(high - new)
            acc, total, high = acc * fade, total * fade, new
        w = jnp.exp(s - high).astype(BF16)
        total = total + jnp.sum(w.astype(F32), axis=0, keepdims=True)
        yield total
        acc = acc + dot(keys(1), w, TN)
        t = jnp.transpose(acc / total)
        t = jnp.where(low, t[:edge], t[edge:])
        rows_of = slice(half * RADIUS, (half + 1) * RADIUS)
        edge_ref[side, rows_of, :, lanes] = t.reshape(RADIUS, RADIUS, d).astype(BF16)

    for n in range(parts):
        run_guarded(functools.partial(unit_of, n), per, 2 * edge, TOGETHER_E)

    copies = []
    for side in range(2):
        g = 0 if side == 0 else groups - 1
        copies.append(
            (edge_ref.at[side], out_ref.at[:, pl.ds(g * RADIUS, RADIUS)])
        )
    started += copy_all(copies, sems.at[pl.ds(2 * parts, 2)])
    for c in started:
        c.wait()


def edges(pg, left, right, corner_up, corner_down, qf, kf, inner, states, scale, tr, tc):
    _, _, _, width = pg.shape
    parts = len(states)
    return pl.pallas_call(
        functools.partial(edge_kernel, scale, parts),
        in_specs=[VMEM] * (7 + 2 * parts),
        out_specs=HBM,
        out_shape=jax.ShapeDtypeStruct((tr, tc, width), BF16),
        scratch_shapes=[
            pltpu.VMEM((2, tr, RADIUS, width), BF16),
            pltpu.SemaphoreType.DMA((2 * parts + 2,)),
        ],
        cost_estimate=pl.CostEstimate(
            flops=500_000_000, bytes_accessed=3_000_000, transcendentals=800_000
        ),
        compiler_params=PARAMS,
        name="edges",
    )(pg, left, right, corner_up, corner_down, qf, kf, *inner, *states)


def local(patches, registers):
    _, tr, tc, width = patches.shape
    groups = tc // RADIUS
    cells = tr * RADIUS
    edge = RADIUS * RADIUS
    assert tr == 2 * RADIUS and groups == 4 and 2 * width == HEADS * LANES
    scale = (width // HEADS) ** (-0.5)
    row_at, row_n = lax.axis_index("row"), lax.axis_size("row")
    col_at, col_n = lax.axis_index("col"), lax.axis_size("col")

    in_vmem = lambda x: pltpu.with_memory_space_constraint(x, pltpu.VMEM)
    pg, to_right, to_left, to_down, to_up = load(patches)
    left = shift(to_right, "col", 1)
    right = shift(to_left, "col", -1)
    up = shift(to_down, "row", 1)
    down = shift(to_up, "row", -1)
    left, right = (x.reshape(2, cells, width) for x in (left, right))
    rows_shape = (2, groups, RADIUS, RADIUS, width)
    up, down = stage(whole, 2, up, down, rows_shape)
    up, down = (x.reshape(2, groups, edge, width) for x in (up, down))

    flag = jnp.where((row_at == 0) & (col_at == 0), 0.0, -1e30).astype(F32).reshape(1)
    pg = pg.reshape(3, groups, cells, width)
    part = prep(pg, registers, flag, scale)

    key_rows = np.repeat(np.arange(-RADIUS, tr + RADIUS), RADIUS)
    key_cols = np.tile(np.arange(RADIUS), tr + 2 * RADIUS)
    stack = lambda cols: np.stack([key_features(key_rows, key_cols + c, tr, tc) for c in cols])
    row = jnp.arange((tr + 2 * RADIUS) * RADIUS, dtype=jnp.int32)[None, :, None]
    off_rows = ((row < edge) & (row_at == 0)) | ((row >= edge + cells) & (row_at == row_n - 1))
    side = jnp.arange(2, dtype=jnp.int32)[:, None, None]
    off_cols = ((side == 0) & (col_at == 0)) | ((side == 1) & (col_at == col_n - 1))
    off_lane = LANES - 1
    kf = with_grid_edge(stack([g * RADIUS for g in range(groups)]), (off_rows, off_lane))
    kf_side = with_grid_edge(stack([-RADIUS, tc]), (off_rows | off_cols, off_lane))
    q_rows = np.repeat(np.arange(tr), RADIUS)
    q_cols = np.tile(np.arange(RADIUS), tr)
    qf = np.stack([query_features(q_rows, q_cols + g * RADIUS, tr, tc) for g in range(groups)])
    qf[..., off_lane] = 1.0
    qf = jnp.asarray(qf.astype(BF16))

    pairs = HEADS // 2
    parts = PARTS
    per = pairs // parts
    done = []
    for n in range(parts):
        done.append(centre(pg, up, down, registers, qf, kf, scale, n * per, per))
    part, first_state = merge_over(part, "row", done[0][1])
    near_l, near_r, first_state, part = lax.optimization_barrier((left, right, first_state, part))
    done[0] = (done[0][0], first_state)
    bottom = jnp.stack([near_l[:, -edge:], near_r[:, -edge:]])
    corner_up = in_vmem(shift(bottom, "row", 1))
    top = jnp.stack([near_l[:, :edge], near_r[:, :edge]])
    corner_down = in_vmem(shift(top, "row", -1))
    part, _ = merge_over(part, "col")
    register_out = (part[0] / part[2]).astype(BF16)
    left, right = stage(whole, 2, near_l, near_r, left.shape)
    inner = [x[0].reshape(2, tr, RADIUS, per * LANES) for x in done]
    states = [x[1] for x in done]
    out = edges(pg, left, right, corner_up, corner_down, qf, kf_side, inner, states, scale, tr, tc)
    return (out, register_out)


def solution(mesh):
    in_specs = (P(None, "row", "col", None), P())
    out_specs = (P("row", "col", None), P())
    return jax.shard_map(local, mesh=mesh, in_specs=in_specs, out_specs=out_specs, check_vma=False)
```
